128 devices in a mesh: model: 4 (over x), data: 32 (over z, y, core).
Axes of the slice: x: 4, y: 4, z: 4, core: 2. Of those that a mesh axis runs over, the one named last changes fastest.
Arguments:
- grad_in: bfloat16 [32, 4, 768, 3072], P('data', None, None, 'model')
- w_in: float32 [4, 768, 3072], P(None, 'data', 'model')
- row_in: float32 [4, 768], P(None, 'data')
- col_in: float32 [4, 3072], P(None, 'model')
- grad_out: bfloat16 [32, 2, 3072, 768], P('data', None, 'model')
- w_out: float32 [2, 3072, 768], P(None, 'model', 'data')
- row_out: float32 [2, 3072], P(None, 'model')
- col_out: float32 [2, 768], P(None, 'data')
- grad_qkv: bfloat16 [32, 9, 768, 768], P('data', None, None, 'model')
- w_qkv: float32 [9, 768, 768], P(None, 'data', 'model')
- row_qkv: float32 [9, 768], P(None, 'data')
- col_qkv: float32 [9, 768], P(None, 'model')
- grad_o: bfloat16 [32, 3, 768, 768], P('data', None, 'model')
- w_o: float32 [3, 768, 768], P(None, 'model', 'data')
- row_o: float32 [3, 768], P(None, 'model')
- col_o: float32 [3, 768], P(None, 'data')
Outputs:
- output 1: float32 [4, 768, 3072], P(None, 'data', 'model')
- output 2: float32 [4, 768], P(None, 'data')
- output 3: float32 [4, 3072], P(None, 'model')
- output 4: float32 [2, 3072, 768], P(None, 'model', 'data')
- output 5: float32 [2, 3072], P(None, 'model')
- output 6: float32 [2, 768], P(None, 'data')
- output 7: float32 [9, 768, 768], P(None, 'data', 'model')
- output 8: float32 [9, 768], P(None, 'data')
- output 9: float32 [9, 768], P(None, 'model')
- output 10: float32 [3, 768, 768], P(None, 'model', 'data')
- output 11: float32 [3, 768], P(None, 'model')
- output 12: float32 [3, 768], P(None, 'data')
All inputs are finite; a program needn't handle non-finite values.
Results may differ from the reference program's by a relative error of at most 0.001.
Values sent between devices are 32-bit elements.
A program may use at most 1 GiB of HBM per device.

```python
import jax
import jax.numpy as jnp
from jax import lax

D = 768
FF = 3072
HEADS = 12
HEAD = 64
LAYERS = 1
DATA_RANKS = 32
OPT_STEP = 4

ATTN_WIDTH = HEADS * HEAD
MATS_IN = 4 * LAYERS
MATS_OUT = 2 * LAYERS
MATS_QKV = 9 * LAYERS
MATS_O = 3 * LAYERS
EPS_SQ = 1e-30
BETA_TWO = 1.0 - OPT_STEP ** -0.8
LR_BASE = min(1e-2, OPT_STEP ** -0.5)


def draw_group(key, count, rows, cols):
    sub_keys = jax.random.split(key, 8)
    row_scale = jnp.exp(jax.random.uniform(sub_keys[0], (count, rows), minval=-1.0, maxval=1.0))
    col_scale = jnp.exp(jax.random.uniform(sub_keys[1], (count, cols), minval=-1.0, maxval=1.0))
    grad_scale = (DATA_RANKS ** 0.5) * row_scale[:, :, None] * col_scale[:, None, :]

    def draw_rank(rank_key):
        return (jax.random.normal(rank_key, (count, rows, cols)) * grad_scale).astype(jnp.bfloat16)

    grad_parts = lax.map(draw_rank, jax.random.split(sub_keys[2], DATA_RANKS))
    level_low = jax.random.uniform(sub_keys[3], (count,), minval=0.02, maxval=0.3)
    level_high = jax.random.uniform(sub_keys[4], (count,), minval=1.5, maxval=3.0)
    mom_level = jnp.where(jnp.arange(count) % 2 == 0, level_low, level_high)
    weight = jax.random.normal(sub_keys[5], (count, rows, cols)) * (rows ** -0.5)
    row_jitter = jax.random.uniform(sub_keys[6], (count, rows), minval=0.5, maxval=1.5)
    col_jitter = jax.random.uniform(sub_keys[7], (count, cols), minval=0.5, maxval=1.5)
    row_mom = (row_scale ** 2) * jnp.mean(col_scale ** 2, axis=1, keepdims=True) * mom_level[:, None] * row_jitter
    col_mom = (col_scale ** 2) * jnp.mean(row_scale ** 2, axis=1, keepdims=True) * mom_level[:, None] * col_jitter
    return grad_parts, weight, row_mom, col_mom


def setup_inputs(seed: int = 0) -> dict:
    sub_keys = jax.random.split(jax.random.key(seed), 4)
    grad_in, w_in, row_in, col_in = draw_group(sub_keys[0], MATS_IN, D, FF)
    grad_out, w_out, row_out, col_out = draw_group(sub_keys[1], MATS_OUT, FF, D)
    grad_qkv, w_qkv, row_qkv, col_qkv = draw_group(sub_keys[2], MATS_QKV, D, ATTN_WIDTH)
    grad_o, w_o, row_o, col_o = draw_group(sub_keys[3], MATS_O, ATTN_WIDTH, D)
    return {'grad_in': grad_in, 'w_in': w_in, 'row_in': row_in, 'col_in': col_in,
            'grad_out': grad_out, 'w_out': w_out, 'row_out': row_out, 'col_out': col_out,
            'grad_qkv': grad_qkv, 'w_qkv': w_qkv, 'row_qkv': row_qkv, 'col_qkv': col_qkv,
            'grad_o': grad_o, 'w_o': w_o, 'row_o': row_o, 'col_o': col_o}


def update_group(grad_parts, weight, row_mom, col_mom):
    grad_mean = jnp.sum(grad_parts, axis=0, dtype=jnp.float32) / DATA_RANKS
    grad_sq = grad_mean * grad_mean + EPS_SQ
    new_row = BETA_TWO * row_mom + (1.0 - BETA_TWO) * jnp.mean(grad_sq, axis=2)
    new_col = BETA_TWO * col_mom + (1.0 - BETA_TWO) * jnp.mean(grad_sq, axis=1)
    row_rel = new_row / jnp.mean(new_row, axis=1, keepdims=True)
    update = grad_mean / jnp.sqrt(row_rel[:, :, None] * new_col[:, None, :])
    upd_rms = jnp.sqrt(jnp.mean(update * update, axis=(1, 2), keepdims=True))
    update = update / jnp.maximum(1.0, upd_rms)
    w_rms = jnp.sqrt(jnp.mean(weight * weight, axis=(1, 2), keepdims=True))
    return weight - LR_BASE * jnp.maximum(1e-3, w_rms) * update, new_row, new_col


def reference(grad_in, w_in, row_in, col_in, grad_out, w_out, row_out, col_out,
              grad_qkv, w_qkv, row_qkv, col_qkv, grad_o, w_o, row_o, col_o):
    w_in_new, row_in_new, col_in_new = update_group(grad_in, w_in, row_in, col_in)
    w_out_new, row_out_new, col_out_new = update_group(grad_out, w_out, row_out, col_out)
    w_qkv_new, row_qkv_new, col_qkv_new = update_group(grad_qkv, w_qkv, row_qkv, col_qkv)
    w_o_new, row_o_new, col_o_new = update_group(grad_o, w_o, row_o, col_o)
    return (w_in_new, row_in_new, col_in_new, w_out_new, row_out_new, col_out_new,
            w_qkv_new, row_qkv_new, col_qkv_new, w_o_new, row_o_new, col_o_new)
```

```python
import jax
import jax.numpy as jnp
from jax import lax
from jax.experimental import pallas as pl
from jax.experimental.pallas import tpu as pltpu
from jax.sharding import PartitionSpec as P

OPT_STEP = 4
EPS_SQ = 1e-30
BETA_TWO = 1.0 - OPT_STEP ** -0.8
LR_BASE = min(1e-2, OPT_STEP ** -0.5)

F32 = jnp.float32
FF = 3072.0
D = 768.0
MESH = pl.DeviceIdType.MESH
RANKS = 32
DIM = 768
THIN = 192
LANES = 128
SECOND = 1024
VEC = 1280
STEPS = 9
PLAIN = 4
HALF = 384
BLK = 24
MATS = 18
WIDE = 6
ROWCUT = (16, 8)

VEC_AT = tuple([(j, 0, DIM) for j in range(6)] + [(j, DIM, THIN) for j in range(8)] + [(j, SECOND, THIN) for j in range(4)])


def kernel(g_in, w_in, r_in, c_in, g_out, w_out, r_out, c_out, g_qkv, w_qkv, r_qkv, c_qkv, g_o, w_o, r_o, c_o,
           w_in_n, r_in_n, c_in_n, w_out_n, r_out_n, c_out_n, w_qkv_n, r_qkv_n, c_qkv_n, w_o_n, r_o_n, c_o_n,
           xin, s0, r0, r1, b2, r2, grad, gsm, pick_f, pick, vw_in, vw_out, vw_qkv, vw_o,
           vr_in, vc_in, vr_out, vc_out, vr_qkv, vc_qkv, vr_o, vc_o,
           square, dv_mom, mv_mom, dv_own, dv_got, mv_own, mv_got, mv_core, mv_rs, sc_own, sc_got, sc_core,
           ld_sem, sm_sem, d2d_s, d2d_r, p1_s, p1_r, p2_s, p2_r,
           dv_s, dv_r, mv_s, mv_r, sc_s, sc_r):
    d = lax.axis_index('data')
    x = lax.axis_index('model')
    core = lax.rem(d, 2)
    y = lax.rem(d // 2, 4)
    z = d // 8

    def at(axis, off):
        if axis == 'x':
            return {'model': lax.rem(x + off, 4)}
        if axis == 'y':
            return {'data': (z * 4 + lax.rem(y + off, 4)) * 2 + core}
        if axis == 'z':
            return {'data': (lax.rem(z + off, 4) * 4 + y) * 2 + core}
        return {'data': (z * 4 + y) * 2 + (1 - core)}

    loads = [pltpu.make_async_copy(g_in.at[k], xin.at[k], ld_sem.at[k]) for k in range(4)]
    loads += [pltpu.make_async_copy(g_out.at[k], xin.at[4 + k], ld_sem.at[4 + k]) for k in range(2)]
    loads += [pltpu.make_async_copy(g_qkv.at[pl.ds(DIM * k, DIM)], xin.at[6 + k], ld_sem.at[6 + k]) for k in range(2)]
    loads += [pltpu.make_async_copy(g_qkv.at[pl.ds(1536, THIN)], xin.at[8, pl.ds(0, THIN)], ld_sem.at[8]),
              pltpu.make_async_copy(g_o, xin.at[8, pl.ds(THIN, 576)], ld_sem.at[STEPS])]
    small = [(w_in, vw_in), (w_out, vw_out), (w_qkv, vw_qkv), (w_o, vw_o), (r_in, vr_in), (c_in, vc_in),
             (r_out, vr_out), (c_out, vc_out), (r_qkv, vr_qkv), (c_qkv, vc_qkv), (r_o, vr_o), (c_o, vc_o)]
    small = [pltpu.make_async_copy(s, t, sm_sem.at[j]) for j, (s, t) in enumerate(small)]
    for cp in loads + small:
        cp.start()

    barrier = pltpu.get_barrier_semaphore()
    peers = [at('c', 1)] + [at(a, j) for a in ('y', 'z', 'x') for j in (1, 2, 3)]
    for p in peers:
        pl.semaphore_signal(barrier, inc=1, device_id=p, device_id_type=MESH)

    for side in range(2):
        cc = (1 - core) if side == 0 else core
        row = lax.broadcasted_iota(jnp.int32, (BLK, HALF), 0)
        col = lax.broadcasted_iota(jnp.int32, (BLK, HALF), 1)
        for b in range(8):
            pick_f[pl.ds(BLK * b, BLK)] = jnp.where(col == row + 48 * b + 24 * cc, 1.0, 0.0)
        pick[side] = pick_f[...].astype(jnp.bfloat16)

    pl.semaphore_wait(barrier, len(peers))

    def remote(src, dst, ss, rs, dev):
        return pltpu.make_async_remote_copy(src_ref=src, dst_ref=dst, send_sem=ss, recv_sem=rs,
                                            device_id=dev, device_id_type=MESH)

    def d2d(k, h):
        return remote(s0.at[k, h], r0.at[k, h], d2d_s.at[k, h], d2d_r.at[k, h], at('c', 1))

    def part(k, side, fn):
        @pl.when(k < PLAIN)
        def _():
            def group(g, carry):
                v = xin[k, pl.ds(pl.multiple_of(48 * g, 16), 48), :].astype(F32)
                first = (core == 0) if side == 1 else (core == 1)
                v = jnp.where(first, v[:BLK], v[BLK:])
                for h in range(2):
                    fn(h, pl.ds(g // 4, 1), pl.ds(lax.rem(g, 4), 1), v[:, HALF * h:HALF * (h + 1)].reshape(1, 1, BLK, HALF))
                return carry
            lax.fori_loop(0, 16, group, 0)

        @pl.when(k >= PLAIN)
        def _():
            def group(g, carry):
                for h in range(2):
                    v = xin[k, pl.ds(HALF * h, HALF), pl.ds(pl.multiple_of(HALF * g, LANES), HALF)]
                    v = lax.dot_general(pick[side], v, (((1,), (1,)), ((), ())), preferred_element_type=F32)
                    fn(h, pl.ds(2 * g, 2), slice(None), v.reshape(2, 4, BLK, HALF))
                return carry
            lax.fori_loop(0, 2, group, 0)

    def stage0(k):
        for j in range(STEPS):
            @pl.when(k == j)
            def _(j=j):
                loads[j].wait()
                if j == 8:
                    loads[STEPS].wait()

        def put(h, zs, ys, v):
            s0[k, h, zs, ys] = v
        part(k, 0, put)
        for h in range(2):
            d2d(k, h).start()

    def ring(h, first):
        axis = ('y', 'z')[h] if first else ('z', 'y')[h]
        return axis, (y if axis == 'y' else z)

    def src1(k, h, t, s):
        return r0.at[k, 0, pl.ds(2 * s, 2), t] if h == 0 else r0.at[k, 1, t, pl.ds(2 * s, 2)]

    def cut(h, s):
        return pl.ds(0, ROWCUT[h]) if s == 0 else pl.ds(ROWCUT[h], BLK - ROWCUT[h])

    def src2(k, h, t, s):
        return b2.at[k, h, t, cut(h, s)]

    def mod4(v):
        return lax.rem(v + 8, 4)

    PLAN = ((-2, 0), (-1, 1), (-1, 0), (2, 1), (1, 0), (1, 1))

    def msg(first, k, h, m):
        axis, n = ring(h, first)
        off, s = PLAN[m]
        t = mod4(n + off)
        dev = at(axis, 3 if m < 3 else 1)
        if first:
            return remote(src1(k, h, t, s), r1.at[k, h, m], p1_s.at[k, h, m], p1_r.at[k, h, m], dev)
        rows = ROWCUT[h] if s == 0 else BLK - ROWCUT[h]
        return remote(src2(k, h, t, s), r2.at[k, h, m, pl.ds(0, rows)], p2_s.at[k, h, m], p2_r.at[k, h, m], dev)

    def got(first, k, h, m):
        if first:
            return r1[k, h, m]
        s = PLAN[m][1]
        return r2[k, h, m, pl.ds(0, ROWCUT[h] if s == 0 else BLK - ROWCUT[h])]

    def send_raw(first, k, h):
        for m in (0, 3, 1, 4):
            msg(first, k, h, m).start()

    def stage1(k):
        for h in range(2):
            d2d(k, h).wait_recv()

        def add(h, zs, ys, v):
            r0[k, h, zs, ys] += v
        part(k, 1, add)
        for h in range(2):
            send_raw(True, k, h)

    def relay(first, k):
        for h in range(2):
            n = ring(h, first)[1]
            for m_in, m_out in ((0, 2), (3, 5)):
                msg(first, k, h, m_in).wait_recv()
                off, s = PLAN[m_out]
                ref = (src1 if first else src2)(k, h, mod4(n + off), s)
                ref[...] += got(first, k, h, m_in)
                msg(first, k, h, m_out).start()

    def stage3(k):
        for h in range(2):
            n = ring(h, True)[1]
            for s, left, right in ((0, 2, 4), (1, 1, 5)):
                msg(True, k, h, left).wait_recv()
                msg(True, k, h, right).wait_recv()
                b2[k, h, pl.ds(2 * s, 2)] = src1(k, h, n, s)[...] + got(True, k, h, left) + got(True, k, h, right)
            send_raw(False, k, h)

    def stage5(k):
        for h in range(2):
            n = ring(h, False)[1]
            for s, left, right in ((0, 2, 4), (1, 1, 5)):
                msg(False, k, h, left).wait_recv()
                msg(False, k, h, right).wait_recv()
                total = src2(k, h, n, s)[...] + got(False, k, h, left) + got(False, k, h, right)
                grad[k, cut(h, s), pl.ds(HALF * h, HALF)] = total / RANKS

    lane = lax.broadcasted_iota(jnp.int32, (1, LANES), 1)

    def put_lane(vec, j, value):
        return jnp.where(lane == j, value, vec)

    def prepare():
        for cp in small:
            cp.wait()
        square[...] = jnp.zeros_like(square)
        square[0:4, 0:BLK] = vr_in[...]
        square[4:6, 0:BLK] = vc_out[...]
        square[6:15, 0:BLK] = vr_qkv[...]
        square[15:18, 0:BLK] = vc_o[...]
        dv_mom[...] = square[...].T[0:BLK]
        mv_mom[...] = jnp.ones_like(mv_mom)
        mv_mom[0:4, 0:DIM] = vc_in[...]
        mv_mom[4:6, 0:DIM] = vr_out[...]
        mv_mom[0:8, DIM:960] = vc_qkv[0:8]
        mv_mom[0:1, SECOND:1216] = vc_qkv[8:STEPS]
        mv_mom[1:4, SECOND:1216] = vr_o[...]
        mv_own[...] = jnp.zeros_like(mv_own)
        sc_own[...] = jnp.zeros_like(sc_own)
        vec = jnp.zeros((1, LANES), F32)
        for j in range(MATS):
            w = weight_of(j)
            vec = put_lane(vec, j, jnp.sum(jnp.sum(w * w, axis=0, keepdims=True), axis=1, keepdims=True))
        sc_own[2:3] = vec

    def weight_of(j):
        return vw_in[j] if j < 4 else vw_out[j - 4] if j < 6 else vw_qkv[j - 6] if j < 15 else vw_o[j - 15]

    def grad_of(j):
        return grad[j] if j < WIDE else gsm[j - WIDE]


    def trip(i, carry):
        for lag, stage in enumerate((stage0, stage1, lambda k: relay(True, k), stage3, lambda k: relay(False, k), stage5)):
            @pl.when(jnp.logical_and(i >= lag, i < STEPS + lag))
            def _(lag=lag, stage=stage):
                stage(i - lag)

        @pl.when(i == 5)
        def _():
            prepare()
        return carry
    lax.fori_loop(0, STEPS + 5, trip, 0)

    for j in range(12):
        k, q = 6 + j // 4, j % 4
        if q % 2 == 0:
            gsm[j] = grad[k, :, THIN * q:THIN * q + THIN]
        else:
            gsm[j] = pltpu.roll(grad[k, :, THIN * q - 64:THIN * q + THIN], THIN, 1)[:, :THIN]

    dv = jnp.zeros((BLK, LANES), F32)
    for j in range(MATS):
        g = grad_of(j)
        s = g * g + EPS_SQ
        dv = jnp.where(lane == j, jnp.sum(s, axis=1, keepdims=True), dv)
        row, at_lane, width = VEC_AT[j]
        mv_own[row:row + 1, at_lane:at_lane + width] = jnp.sum(s, axis=0, keepdims=True)
    dv_own[...] = dv

    def spread(axis, src, dst, ss, rs):
        return [remote(src, dst.at[j], ss.at[j], rs.at[j], at(axis, j)) for j in (1, 2, 3)]

    def collect(src, dst, copies):
        for cp in copies:
            cp.wait_recv()
        return (src[...] + dst[2]) + (dst[1] + dst[3])

    dv_cp = spread('x', dv_own, dv_got, dv_s, dv_r)
    for cp in dv_cp:
        cp.start()
    core_cp = remote(mv_own, mv_core.at[0], mv_s.at[0, 0], mv_r.at[0, 0], at('c', 1))
    core_cp.start()
    core_cp.wait_recv()
    mv_core[1] = mv_own[...] + mv_core[0]
    y_cp = spread('y', mv_core.at[1], mv_got.at[0], mv_s.at[1], mv_r.at[1])
    for cp in y_cp:
        cp.start()
    count = jnp.where(lane < WIDE, FF, D)
    dv_new = BETA_TWO * dv_mom[...] + (1.0 - BETA_TWO) * (collect(dv_own, dv_got, dv_cp) / count)
    dv_inv = 1.0 / jnp.sqrt(jnp.where(lane < MATS, dv_new, 1.0))
    square[0:BLK] = dv_new
    turned = square[...].T
    r_in_n[...] = turned[0:4, 0:BLK]
    c_out_n[...] = turned[4:6, 0:BLK]
    r_qkv_n[...] = turned[6:15, 0:BLK]
    c_o_n[...] = turned[15:18, 0:BLK]
    for j in range(MATS):
        g = grad_of(j) * dv_inv[:, j:j + 1]
        if j < WIDE:
            grad[j] = g
        else:
            gsm[j - WIDE] = g
    mv_core[2] = collect(mv_core.at[1], mv_got.at[0], y_cp)
    z_cp = spread('z', mv_core.at[2], mv_got.at[1], mv_s.at[2], mv_r.at[2])
    for cp in z_cp:
        cp.start()
    mv_sum = collect(mv_core.at[2], mv_got.at[1], z_cp)
    mv_new = BETA_TWO * mv_mom[...] + (1.0 - BETA_TWO) * (mv_sum / D)
    mv_mom[...] = mv_new
    c_in_n[...] = mv_mom[0:4, 0:DIM]
    r_out_n[...] = mv_mom[4:6, 0:DIM]
    c_qkv_n[0:8] = mv_mom[0:8, DIM:960]
    c_qkv_n[8:STEPS] = mv_mom[0:1, SECOND:1216]
    r_o_n[...] = mv_mom[1:4, SECOND:1216]
    mv_inv = 1.0 / jnp.sqrt(mv_new)
    mv_rs[...] = mv_inv

    upd_vec = jnp.zeros((1, LANES), F32)
    row_vec = jnp.sum(dv_new, axis=0, keepdims=True) / 4
    for j in range(MATS):
        row, at_lane, width = VEC_AT[j]
        u = grad_of(j) * mv_rs[row:row + 1, at_lane:at_lane + width]
        if j < WIDE:
            grad[j] = u
        else:
            gsm[j - WIDE] = u
        upd_vec = put_lane(upd_vec, j, jnp.sum(jnp.sum(u * u, axis=0, keepdims=True), axis=1, keepdims=True))
        if 4 <= j < 6 or j >= 15:
            row_vec = put_lane(row_vec, j, jnp.sum(mv_mom[row:row + 1, at_lane:at_lane + width], axis=1, keepdims=True) / 32)
    sc_own[0:1] = upd_vec
    sc_own[1:2] = row_vec

    core_sc = remote(sc_own, sc_core.at[0], sc_s.at[0, 0], sc_r.at[0, 0], at('c', 1))
    core_sc.start()
    core_sc.wait_recv()
    sc_core[1] = sc_own[...] + sc_core[0]
    sc_cp = []
    for n, axis in enumerate(('y', 'z', 'x')):
        cps = spread(axis, sc_core.at[n + 1], sc_got.at[n], sc_s.at[n + 1], sc_r.at[n + 1])
        for cp in cps:
            cp.start()
        sc_cp += cps
        sc_core[n + 2] = collect(sc_core.at[n + 1], sc_got.at[n], cps)
    full = jnp.where(lane < WIDE, FF * D, D * D)
    rows = jnp.where(jnp.logical_and(lane >= 4, lane < 6), FF, D)
    row_mean = sc_core[4, 1:2] / rows
    upd_rms = jnp.sqrt(row_mean * (sc_core[4, 0:1] / full))
    w_rms = jnp.sqrt(sc_core[4, 2:3] / full)
    scale = LR_BASE * jnp.maximum(1e-3, w_rms) * (jnp.sqrt(row_mean) / jnp.maximum(1.0, upd_rms))
    for j in range(MATS):
        new = weight_of(j) - scale[:, j:j + 1] * grad_of(j)
        if j < 4:
            w_in_n[j] = new
        elif j < 6:
            w_out_n[j - 4] = new
        elif j < 15:
            w_qkv_n[j - 6] = new
        else:
            w_o_n[j - 15] = new

    def drain(k, carry):
        for h in range(2):
            d2d(k, h).wait_send()
            for m in range(6):
                msg(True, k, h, m).wait_send()
                msg(False, k, h, m).wait_send()
        return carry
    lax.fori_loop(0, STEPS, drain, 0)
    for cp in dv_cp + [core_cp] + y_cp + z_cp + [core_sc] + sc_cp:
        cp.wait_send()


def write_out(*refs):
    n = len(refs) // 2
    copies = [pltpu.make_async_copy(refs[j], refs[n + j], refs[-1].at[j]) for j in range(n)]
    for cp in copies:
        cp.start()
    for cp in copies:
        cp.wait()


def solution(mesh):
    rows_data = (P('data', None, None, 'model'), P(None, 'data', 'model'), P(None, 'data'), P(None, 'model'))
    rows_model = (P('data', None, 'model', None), P(None, 'model', 'data'), P(None, 'model'), P(None, 'data'))
    DMA = pltpu.SemaphoreType.DMA

    def step_all(grad_in, w_in, row_in, col_in, grad_out, w_out, row_out, col_out,
                 grad_qkv, w_qkv, row_qkv, col_qkv, grad_o, w_o, row_o, col_o):
        args = (grad_in[0], w_in, row_in, col_in,
                grad_out[0], w_out.swapaxes(1, 2), row_out, col_out,
                grad_qkv[0].swapaxes(1, 2).reshape(1728, DIM), w_qkv, row_qkv, col_qkv,
                grad_o[0].reshape(576, DIM), w_o.swapaxes(1, 2), row_o, col_o)
        small = [a for n, a in enumerate(args) if n % 4]
        outs = [jax.ShapeDtypeStruct(a.shape, a.dtype) for a in small]
        held = [pltpu.VMEM(a.shape, a.dtype) for a in small]
        vm = lambda *s: pltpu.VMEM(s, F32)
        res = pl.pallas_call(
            kernel,
            out_shape=held,
            in_specs=[pl.BlockSpec(memory_space=pl.ANY)] * len(args),
            out_specs=[pl.BlockSpec(memory_space=pltpu.VMEM)] * len(outs),
            scratch_shapes=[
                pltpu.VMEM((STEPS, DIM, DIM), jnp.bfloat16),
                vm(STEPS, 2, 4, 4, BLK, HALF), vm(STEPS, 2, 4, 4, BLK, HALF),
                vm(STEPS, 2, 6, 2, BLK, HALF), vm(STEPS, 2, 4, BLK, HALF), vm(STEPS, 2, 6, 16, HALF),
                vm(STEPS, BLK, DIM), vm(12, BLK, THIN),
                vm(THIN, HALF), pltpu.VMEM((2, THIN, HALF), jnp.bfloat16),
                vm(4, BLK, DIM), vm(2, BLK, DIM), vm(STEPS, BLK, THIN), vm(3, BLK, THIN),
                vm(4, BLK), vm(4, DIM), vm(2, DIM), vm(2, BLK), vm(STEPS, BLK), vm(STEPS, THIN), vm(3, THIN), vm(3, BLK),
                vm(LANES, LANES), vm(BLK, LANES), vm(8, VEC),
                vm(BLK, LANES), vm(4, BLK, LANES), vm(8, VEC), vm(2, 4, 8, VEC), vm(3, 8, VEC), vm(8, VEC),
                vm(8, LANES), vm(3, 4, 8, LANES), vm(5, 8, LANES),
                DMA((10,)), DMA((12,)), DMA((STEPS, 2)), DMA((STEPS, 2)),
                DMA((STEPS, 2, 6)), DMA((STEPS, 2, 6)), DMA((STEPS, 2, 6)), DMA((STEPS, 2, 6)),
                DMA((4,)), DMA((4,)), DMA((3, 4)), DMA((3, 4)), DMA((4, 4)), DMA((4, 4)),
            ],
            compiler_params=pltpu.CompilerParams(
                collective_id=0, has_side_effects=True, vmem_limit_bytes=58_000_000),
            name='adafactor',
        )(*args)
        res = list(pl.pallas_call(
            write_out,
            out_shape=outs,
            in_specs=[pl.BlockSpec(memory_space=pltpu.VMEM)] * len(outs),
            out_specs=[pl.BlockSpec(memory_space=pl.ANY)] * len(outs),
            scratch_shapes=[DMA((len(outs),))],
            name='write_out',
        )(*[pltpu.with_memory_space_constraint(r, pltpu.VMEM) for r in res]))
        for n in (3, STEPS):
            res[n] = res[n].swapaxes(1, 2)
        return tuple(res)

    in_specs = rows_data + rows_model + rows_data + rows_model
    out_specs = rows_data[1:] + rows_model[1:] + rows_data[1:] + rows_model[1:]
    return jax.shard_map(step_all, mesh=mesh, in_specs=in_specs, out_specs=out_specs, check_vma=False)
```

```python
import jax
import jax.numpy as jnp
from jax import lax
from jax.experimental import pallas as pl
from jax.experimental.pallas import tpu as pltpu
from jax.sharding import PartitionSpec as P

OPT_STEP = 4
EPS_SQ = 1e-30
BETA_TWO = 1.0 - OPT_STEP ** -0.8
LR_BASE = min(1e-2, OPT_STEP ** -0.5)

F32 = jnp.float32
MESH = pl.DeviceIdType.MESH
FF, D = 3072.0, 768.0
DIM = 768
THIN = 192
LANES = 128
PAIR = 256
SLABS = 9
PLAIN = 4
WIDE = 6
MATS = 18
CUTS = 1
STEPS = SLABS * CUTS
HALF = 384
CW = HALF // CUTS
BLK = 24
ROWCUT = (16, 8)
UP = 2.0 ** 48

LAG_ADD, LAG_RELAY1, LAG_TURN, LAG_RELAY2, LAG_SUM = 1, 2, 3, 4, 5
LAG_DV, LAG_CORE, LAG_Y, LAG_Z = 6, 7, 8, 9


def mod4(v):
    return lax.rem(v + 8, 4)


def cut(h, s):
    return pl.ds(0, ROWCUT[h]) if s == 0 else pl.ds(ROWCUT[h], BLK - ROWCUT[h])


def kernel(g_in, w_in, r_in, c_in, g_out, w_out, r_out, c_out, g_qkv, w_qkv, r_qkv, c_qkv, g_o, w_o, r_o, c_o,
           w_in_n, r_in_n, c_in_n, w_out_n, r_out_n, c_out_n, w_qkv_n, r_qkv_n, c_qkv_n, w_o_n, r_o_n, c_o_n,
           xin, s0, r0, r1a, r1b, b2, r2a, r2b, grad, gsm, pick_f, pick, vw_in, vw_out, vw_qkv, vw_o,
           vr_in, vc_in, vr_out, vc_out, vr_qkv, vc_qkv, vr_o, vc_o,
           square, thin_a, thin_b, dv_mom, dv_all, dv_own, dv_got, mv_mom, mv_new, mv_own, mv_core, mv_one, mv_y, mv_two, mv_z,
           sc_own, sc_got, ld_sem, sm_sem, d2d_s, d2d_r, p1_s, p1_r, p2_s, p2_r, dv_s, dv_r, mv_s, mv_r, sc_s, sc_r):
    d = lax.axis_index('data')
    x = lax.axis_index('model')
    core = lax.rem(d, 2)
    y = lax.rem(d // 2, 4)
    z = d // 8

    def at(axis, off):
        if axis == 'x':
            return {'model': lax.rem(x + off, 4)}
        if axis == 'y':
            return {'data': (z * 4 + lax.rem(y + off, 4)) * 2 + core}
        if axis == 'z':
            return {'data': (lax.rem(z + off, 4) * 4 + y) * 2 + core}
        return {'data': (z * 4 + y) * 2 + (1 - core)}

    def local(src, dst, sem):
        return pltpu.make_async_copy(src, dst, sem)

    loads = [local(g_in.at[k], xin.at[k], ld_sem.at[k]) for k in range(PLAIN)]
    loads += [local(g_out.at[k - PLAIN], xin.at[k], ld_sem.at[k]) for k in range(PLAIN, WIDE)]
    loads += [local(g_qkv.at[pl.ds(DIM * k, DIM)], xin.at[WIDE + k], ld_sem.at[WIDE + k]) for k in range(2)]
    loads += [local(g_qkv.at[pl.ds(2 * DIM, THIN)], xin.at[SLABS - 1, pl.ds(0, THIN)], ld_sem.at[SLABS - 1]),
              local(g_o, xin.at[SLABS - 1, pl.ds(THIN, DIM - THIN)], ld_sem.at[SLABS])]
    small = [(w_in, vw_in), (w_out, vw_out), (w_qkv, vw_qkv), (w_o, vw_o), (r_in, vr_in), (c_in, vc_in),
             (r_out, vr_out), (c_out, vc_out), (r_qkv, vr_qkv), (c_qkv, vc_qkv), (r_o, vr_o), (c_o, vc_o)]
    small = [local(s, t, sm_sem.at[j]) for j, (s, t) in enumerate(small)]
    for cp in loads + small:
        cp.start()

    barrier = pltpu.get_barrier_semaphore()
    peers = [at('c', 1)] + [at(a, j) for a in 'yzx' for j in (1, 2, 3)]
    for p in peers:
        pl.semaphore_signal(barrier, inc=1, device_id=p, device_id_type=MESH)
    pl.semaphore_wait(barrier, len(peers))

    def remote(src, dst, ss, rs, dev):
        return pltpu.make_async_remote_copy(src_ref=src, dst_ref=dst, send_sem=ss, recv_sem=rs,
                                            device_id=dev, device_id_type=MESH)

    def d2d(s, h):
        return remote(s0.at[s, h], r0.at[s, h], d2d_s.at[s, h], d2d_r.at[s, h], at('c', 1))

    def make_pick():
        for side in range(2):
            cc = (1 - core) if side == 0 else core
            row = lax.broadcasted_iota(jnp.int32, (BLK, HALF), 0)
            col = lax.broadcasted_iota(jnp.int32, (BLK, HALF), 1)
            for b in range(8):
                pick_f[pl.ds(BLK * b, BLK)] = jnp.where(col == row + 2 * BLK * b + BLK * cc, 1.0, 0.0)
            pick[side] = pick_f[...].astype(jnp.bfloat16)

    def part(s, side, fn):
        k = s // CUTS
        start = CW * lax.rem(s, CUTS)

        @pl.when(k < PLAIN)
        def _():
            first = (core == 0) if side == 1 else (core == 1)
            for g in range(16):
                for h in range(2):
                    v = xin[k, pl.ds(2 * BLK * g, 2 * BLK), pl.ds(pl.multiple_of(start + HALF * h, LANES), CW)].astype(F32)
                    fn(h, pl.ds(g // 4, 1), pl.ds(g % 4, 1), jnp.where(first, v[:BLK], v[BLK:]).reshape(1, 1, BLK, CW))

        @pl.when(k >= PLAIN)
        def _():
            for g in range(2):
                for h in range(2):
                    v = xin[k, pl.ds(pl.multiple_of(start + HALF * h, LANES), CW), pl.ds(HALF * g, HALF)]
                    v = lax.dot_general(pick[side], v, (((1,), (1,)), ((), ())), preferred_element_type=F32)
                    fn(h, pl.ds(2 * g, 2), slice(None), v.reshape(2, 4, BLK, CW))

    def stage_split(s):
        for j in range(SLABS):
            @pl.when(s == j * CUTS)
            def _(j=j):
                loads[j].wait()
                if j == SLABS - 1:
                    loads[SLABS].wait()

        def put(h, zs, ys, v):
            s0[s, h, zs, ys] = v
        part(s, 0, put)
        for h in range(2):
            d2d(s, h).start()

    def ring(h, first):
        axis = ('y', 'z')[h] if first else ('z', 'y')[h]
        return axis, (y if axis == 'y' else z)

    def block(first, s, h, t, piece):
        if not first:
            return b2.at[s, h, t, cut(h, piece)]
        return r0.at[s, 0, pl.ds(2 * piece, 2), t] if h == 0 else r0.at[s, 1, t, pl.ds(2 * piece, 2)]

    def landing(first, h, piece):
        return pl.ds(2 * piece, 2) if first else cut(h, piece)

    PLAN = ((-2, 0, 0), (2, 1, 1), (-1, 1, 0), (1, 0, 1), (-1, 0, 0), (1, 1, 1))

    def msg(first, s, h, m):
        axis, n = ring(h, first)
        off, piece, way = PLAN[m]
        send, recv, relayed, landed = (p1_s, p1_r, r1a, r1b) if first else (p2_s, p2_r, r2a, r2b)
        src = block(first, s, h, mod4(n + off), piece)
        if m < 2:
            dst = relayed.at[s, h, way] if first else relayed.at[s, h, way, pl.ds(0, cut(h, piece).size)]
        else:
            dst = landed.at[s, h, way, landing(first, h, piece)]
        return remote(src, dst, send.at[s, h], recv.at[s, h, min(m, 2)], at(axis, 1 if way else 3))

    def send_raw(first, s, h):
        for m in range(4):
            msg(first, s, h, m).start()

    def stage_add(s):
        for h in range(2):
            d2d(s, h).wait_recv()

        def add(h, zs, ys, v):
            r0[s, h, zs, ys] += v
        part(s, 1, add)
        for h in range(2):
            send_raw(True, s, h)

    def relay(first, s):
        for h in range(2):
            n = ring(h, first)[1]
            for m in range(2):
                msg(first, s, h, m).wait_recv()
                off, piece, way = PLAN[4 + m]
                ref = block(first, s, h, mod4(n + off), piece)
                if first:
                    ref[...] += r1a[s, h, way]
                else:
                    ref[...] += r2a[s, h, way, pl.ds(0, cut(h, piece).size)]
                msg(first, s, h, 4 + m).start()

    def wait_landed(first, s, h):
        landed, recv = (r1b, p1_r) if first else (r2b, p2_r)
        local(landed.at[s, h], landed.at[s, h], recv.at[s, h, 2]).wait()

    def stage_turn(s):
        for h in range(2):
            n = ring(h, True)[1]
            wait_landed(True, s, h)
            own = r0[s, 0, :, n] if h == 0 else r0[s, 1, n]
            b2[s, h] = own + r1b[s, h, 0] + r1b[s, h, 1]
            send_raw(False, s, h)

    def stage_sum(s):
        k = s // CUTS
        start = CW * lax.rem(s, CUTS)
        for h in range(2):
            n = ring(h, False)[1]
            wait_landed(False, s, h)
            total = b2[s, h, n] + r2b[s, h, 0] + r2b[s, h, 1]
            grad[k, :, pl.ds(pl.multiple_of(start + HALF * h, LANES), CW)] = total / 32

    lane = lax.broadcasted_iota(jnp.int32, (1, LANES), 1)
    col = lax.broadcasted_iota(jnp.int32, (1, DIM), 1)
    count = jnp.where(lane < WIDE, FF, D)

    def of_mat(q):
        return jnp.logical_and(col >= THIN * q, col < THIN * q + THIN)

    def total(v):
        return jnp.sum(jnp.sum(v, axis=0, keepdims=True), axis=1, keepdims=True)

    def weight_of(j):
        return vw_in[j] if j < 4 else vw_out[j - 4] if j < 6 else vw_qkv[j - 6] if j < 15 else vw_o[j - 15]

    def prepare():
        for cp in small:
            cp.wait()
        make_pick()
        square[...] = jnp.zeros_like(square)
        square[0:4, 0:BLK] = vr_in[...]
        square[4:6, 0:BLK] = vc_out[...]
        square[6:15, 0:BLK] = vr_qkv[...]
        square[15:18, 0:BLK] = vc_o[...]
        dv_mom[...] = square[...].T[0:BLK]
        thin_a[...] = jnp.zeros_like(thin_a)
        thin_a[0:9, 0:THIN] = vc_qkv[...]
        thin_a[9:12, 0:THIN] = vr_o[...]
        thin_b[...] = pltpu.roll(thin_a[...], 64, 1)
        for k in range(4):
            mv_mom[k] = vc_in[k:k + 1]
        for k in range(2):
            mv_mom[4 + k] = vr_out[k:k + 1]
        for j in range(12):
            k, q = WIDE + j // 4, j % 4
            if q % 2 == 0:
                mv_mom[k, :, THIN * q:THIN * q + THIN] = thin_a[j:j + 1, 0:THIN]
            else:
                span = slice(THIN * q - 64, THIN * q + THIN)
                mv_mom[k, :, span] = jnp.where(col[:, :PAIR] < 64, mv_mom[k, :, span], thin_b[j:j + 1])
        mv_own[...] = jnp.zeros_like(mv_own)
        sc_own[...] = jnp.zeros_like(sc_own)
        dv_all[...] = jnp.ones_like(dv_all)
        vec = jnp.zeros((1, LANES), F32)
        for j in range(MATS):
            w = weight_of(j)
            vec = jnp.where(lane == j, total(w * w), vec)
        mv_own[SLABS - 1, 2:3, LANES:PAIR] = vec

    def spread(axis, src, dst, ss, rs):
        return [remote(src, dst.at[j], ss.at[j], rs.at[j], at(axis, j)) for j in (1, 2, 3)]

    def start(copies):
        for cp in copies:
            cp.start()

    def collect(src, dst, copies):
        for cp in copies:
            cp.wait_recv()
        return (src[...] + dst[2]) + (dst[1] + dst[3])

    def dv_copies(k):
        return spread('x', dv_own.at[k], dv_got.at[k], dv_s.at[k], dv_r.at[k])

    def core_copy(k):
        return remote(mv_own.at[k], mv_core.at[k], mv_s.at[0, k, 0], mv_r.at[0, k, 0], at('c', 1))

    def y_copies(k):
        return spread('y', mv_one.at[k], mv_y.at[k], mv_s.at[1, k], mv_r.at[1, k])

    def z_copies(k):
        return spread('z', mv_two.at[k], mv_z.at[k], mv_s.at[2, k], mv_r.at[2, k])

    def sums(k):
        g = grad[k]
        s = g * g + EPS_SQ
        mv_own[k, 0:1] = jnp.sum(s, axis=0, keepdims=True)

        @pl.when(k < WIDE)
        def _():
            dv_own[k] = jnp.where(lane == k, jnp.sum(s, axis=1, keepdims=True), 0.0)

        @pl.when(k >= WIDE)
        def _():
            dv = jnp.zeros((BLK, LANES), F32)
            for q in range(4):
                dv = jnp.where(lane == 4 * k - 18 + q, jnp.sum(jnp.where(of_mat(q), s, 0.0), axis=1, keepdims=True), dv)
            dv_own[k] = dv
        start(dv_copies(k))

    def mats_of(k):
        low = jnp.where(k < WIDE, k, 4 * k - 18)
        return jnp.logical_and(lane >= low, lane < jnp.where(k < WIDE, k + 1, 4 * k - 14))

    def data_side(k):
        mine = mats_of(k)
        new = BETA_TWO * dv_mom[...] + (1.0 - BETA_TWO) * (collect(dv_own.at[k], dv_got.at[k], dv_copies(k)) / count)
        dv_all[...] = jnp.where(mine, new, dv_all[...])
        mv_own[k, 2:3, 0:LANES] = jnp.where(mine, jnp.sum(new, axis=0, keepdims=True), 0.0)
        inv = 1.0 / jnp.sqrt(jnp.where(mine, new, 1.0))

        def column(j):
            return jnp.sum(jnp.where(lane == j, inv, 0.0), axis=1, keepdims=True)

        def scaled(factor):
            q = grad[k] * factor
            grad[k] = q
            q = q * UP
            mv_own[k, 1:2] = jnp.sum(q * q, axis=0, keepdims=True)

        @pl.when(k < WIDE)
        def _():
            scaled(column(k))

        @pl.when(k >= WIDE)
        def _():
            factor = column(4 * k - 15)
            for q in (2, 1, 0):
                factor = jnp.where(col < THIN * q + THIN, column(4 * k - 18 + q), factor)
            scaled(factor)
        core_copy(k).start()

    def stage_y(k):
        core_copy(k).wait_recv()
        mv_one[k] = mv_own[k] + mv_core[k]
        start(y_copies(k))

    def stage_z(k):
        mv_two[k] = collect(mv_one.at[k], mv_y.at[k], y_copies(k))
        start(z_copies(k))

    def model_side(k):
        mine = mats_of(k)
        v = collect(mv_two.at[k], mv_z.at[k], z_copies(k))
        new = BETA_TWO * mv_mom[k] + (1.0 - BETA_TWO) * (v[0:1] / D)
        mv_new[k] = new
        inv = 1.0 / jnp.sqrt(new)
        a = jnp.sqrt(v[1:2]) * inv * (1.0 / UP)
        a = a * a
        u = grad[k] * inv
        rows = jnp.where(mine, v[2:3, 0:LANES] / 4, sc_own[1:2])

        @pl.when(k < WIDE)
        def _():
            sc_own[0:1] = jnp.where(mine, total(a), sc_own[0:1])
            sc_own[1:2] = jnp.where(jnp.logical_and(mine, lane >= 4), total(new), rows)
            grad[k] = u

        @pl.when(k >= WIDE)
        def _():
            upd, row = sc_own[0:1], rows
            for q in range(4):
                j = 4 * k - 18 + q
                upd = jnp.where(lane == j, total(jnp.where(of_mat(q), a, 0.0)), upd)
                row = jnp.where(jnp.logical_and(lane == j, lane >= 15), total(jnp.where(of_mat(q), new, 0.0)), row)
                if q % 2 == 0:
                    gsm[j - WIDE] = u[:, THIN * q:THIN * q + THIN]
                else:
                    gsm[j - WIDE] = pltpu.roll(u[:, THIN * q - 64:THIN * q + THIN], THIN, 1)[:, :THIN]
            sc_own[0:1] = upd
            sc_own[1:2] = row
            sc_own[2:3] = v[2:3, LANES:PAIR]

    stages = ((0, stage_split), (LAG_ADD, stage_add), (LAG_RELAY1, lambda s: relay(True, s)), (LAG_TURN, stage_turn),
              (LAG_RELAY2, lambda s: relay(False, s)), (LAG_SUM, stage_sum))
    slab_stages = ((LAG_SUM, sums), (LAG_DV, data_side), (LAG_CORE, stage_y), (LAG_Y, stage_z), (LAG_Z, model_side))

    def trip(i, carry):
        for lag, stage in stages:
            @pl.when(jnp.logical_and(i >= lag, i < STEPS + lag))
            def _(lag=lag, stage=stage):
                stage(i - lag)

        @pl.when(i == LAG_RELAY1)
        def _():
            prepare()
        for lag, stage in slab_stages:
            e = i - lag - (CUTS - 1)

            @pl.when(jnp.logical_and(jnp.logical_and(e >= 0, e < STEPS), lax.rem(e + STEPS, CUTS) == 0))
            def _(e=e, stage=stage):
                stage(e // CUTS)
        return carry
    lax.fori_loop(0, STEPS + LAG_Z, trip, 0)

    sc_cp = spread('x', sc_own, sc_got, sc_s, sc_r)
    start(sc_cp)

    square[0:BLK] = dv_all[...]
    turned = square[...].T
    r_in_n[...] = turned[0:4, 0:BLK]
    c_out_n[...] = turned[4:6, 0:BLK]
    r_qkv_n[...] = turned[6:15, 0:BLK]
    c_o_n[...] = turned[15:18, 0:BLK]
    for k in range(4):
        c_in_n[k:k + 1] = mv_new[k]
    for k in range(2):
        r_out_n[k:k + 1] = mv_new[4 + k]
    for j in range(12):
        k, q = WIDE + j // 4, j % 4
        if q % 2 == 0:
            thin_a[j:j + 1, 0:THIN] = mv_new[k, :, THIN * q:THIN * q + THIN]
        else:
            thin_b[j:j + 1] = mv_new[k, :, THIN * q - 64:THIN * q + THIN]
    odd = lax.rem(lax.broadcasted_iota(jnp.int32, thin_a.shape, 0), 2) == 1
    thin_a[...] = jnp.where(odd, pltpu.roll(thin_b[...], THIN, 1), thin_a[...])
    c_qkv_n[...] = thin_a[0:9, 0:THIN]
    r_o_n[...] = thin_a[9:12, 0:THIN]

    def drain(s, carry):
        for h in range(2):
            d2d(s, h).wait_send()
            for buf, sem in ((s0.at[s, h, pl.ds(0, 3)], p1_s), (b2.at[s, h, pl.ds(0, 3)], p2_s)):
                local(buf, buf, sem.at[s, h]).wait()
        return carry
    lax.fori_loop(0, STEPS, drain, 0)

    def drain_slab(k, carry):
        for cp in dv_copies(k) + [core_copy(k)] + y_copies(k) + z_copies(k):
            cp.wait_send()
        return carry
    lax.fori_loop(0, SLABS, drain_slab, 0)

    sc = collect(sc_own, sc_got, sc_cp)
    full = jnp.where(lane < WIDE, FF * D, D * D)
    rows = jnp.where(jnp.logical_and(lane >= 4, lane < 6), FF, D)
    row_mean = sc[1:2] / rows
    upd_rms = jnp.sqrt(row_mean * (sc[0:1] / full))
    w_rms = jnp.sqrt(sc[2:3] / full)
    scale = LR_BASE * jnp.maximum(1e-3, w_rms) * (jnp.sqrt(row_mean) / jnp.maximum(1.0, upd_rms))
    for j in range(MATS):
        upd = grad[j] if j < WIDE else gsm[j - WIDE]
        new = weight_of(j) - scale[:, j:j + 1] * upd
        if j < 4:
            w_in_n[j] = new
        elif j < 6:
            w_out_n[j - 4] = new
        elif j < 15:
            w_qkv_n[j - 6] = new
        else:
            w_o_n[j - 15] = new
    for cp in sc_cp:
        cp.wait_send()


def write_out(*refs):
    n = len(refs) // 2
    copies = [pltpu.make_async_copy(refs[j], refs[n + j], refs[-1].at[j]) for j in range(n)]
    for cp in copies:
        cp.start()
    for cp in copies:
        cp.wait()


def solution(mesh):
    rows_data = (P('data', None, None, 'model'), P(None, 'data', 'model'), P(None, 'data'), P(None, 'model'))
    rows_model = (P('data', None, 'model', None), P(None, 'model', 'data'), P(None, 'model'), P(None, 'data'))
    DMA = pltpu.SemaphoreType.DMA

    def step_all(grad_in, w_in, row_in, col_in, grad_out, w_out, row_out, col_out,
                 grad_qkv, w_qkv, row_qkv, col_qkv, grad_o, w_o, row_o, col_o):
        args = (grad_in[0], w_in, row_in, col_in,
                grad_out[0], w_out.swapaxes(1, 2), row_out, col_out,
                grad_qkv[0].swapaxes(1, 2).reshape(-1, DIM), w_qkv, row_qkv, col_qkv,
                grad_o[0].reshape(-1, DIM), w_o.swapaxes(1, 2), row_o, col_o)
        small = [a for n, a in enumerate(args) if n % 4]
        outs = [jax.ShapeDtypeStruct(a.shape, a.dtype) for a in small]
        held = [pltpu.VMEM(a.shape, a.dtype) for a in small]
        vm = lambda *s: pltpu.VMEM(s, F32)
        res = pl.pallas_call(
            kernel,
            out_shape=held,
            in_specs=[pl.BlockSpec(memory_space=pl.ANY)] * len(args),
            out_specs=[pl.BlockSpec(memory_space=pltpu.VMEM)] * len(outs),
            scratch_shapes=[
                pltpu.VMEM((SLABS, DIM, DIM), jnp.bfloat16),
                vm(STEPS, 2, 4, 4, BLK, CW), vm(STEPS, 2, 4, 4, BLK, CW),
                vm(STEPS, 2, 2, 2, BLK, CW), vm(STEPS, 2, 2, 4, BLK, CW), vm(STEPS, 2, 4, BLK, CW),
                vm(STEPS, 2, 2, 16, CW), vm(STEPS, 2, 2, BLK, CW),
                vm(SLABS, BLK, DIM), vm(12, BLK, THIN),
                vm(THIN, HALF), pltpu.VMEM((2, THIN, HALF), jnp.bfloat16)]
            + [vm(*a.shape) for n, a in enumerate(small) if n % 3 == 0] + [vm(*a.shape) for n, a in enumerate(small) if n % 3]
            + [vm(LANES, LANES), vm(16, PAIR), vm(16, PAIR), vm(BLK, LANES), vm(BLK, LANES),
               vm(SLABS, BLK, LANES), vm(SLABS, 4, BLK, LANES), vm(SLABS, 1, DIM), vm(SLABS, 1, DIM),
               vm(SLABS, 4, DIM), vm(SLABS, 4, DIM), vm(SLABS, 4, DIM), vm(SLABS, 4, 4, DIM), vm(SLABS, 4, DIM),
               vm(SLABS, 4, 4, DIM), vm(8, LANES), vm(4, 8, LANES),
               DMA((SLABS + 1,)), DMA((len(small),)), DMA((STEPS, 2)), DMA((STEPS, 2)),
               DMA((STEPS, 2)), DMA((STEPS, 2, 3)), DMA((STEPS, 2)), DMA((STEPS, 2, 3)),
               DMA((SLABS, 4)), DMA((SLABS, 4)), DMA((3, SLABS, 4)), DMA((3, SLABS, 4)), DMA((4,)), DMA((4,))],
            compiler_params=pltpu.CompilerParams(
                collective_id=0, has_side_effects=True, vmem_limit_bytes=58_000_000),
            name='adafactor',
        )(*args)
        res = list(pl.pallas_call(
            write_out,
            out_shape=outs,
            in_specs=[pl.BlockSpec(memory_space=pltpu.VMEM)] * len(outs),
            out_specs=[pl.BlockSpec(memory_space=pl.ANY)] * len(outs),
            scratch_shapes=[DMA((len(outs),))],
            name='write_out',
        )(*[pltpu.with_memory_space_constraint(r, pltpu.VMEM) for r in res]))
        for n in (3, SLABS):
            res[n] = res[n].swapaxes(1, 2)
        return tuple(res)

    in_specs = rows_data + rows_model + rows_data + rows_model
    out_specs = rows_data[1:] + rows_model[1:] + rows_data[1:] + rows_model[1:]
    return jax.shard_map(step_all, mesh=mesh, in_specs=in_specs, out_specs=out_specs, check_vma=False)
```

```python
import jax
import jax.numpy as jnp
from jax import lax
from jax.experimental import pallas as pl
from jax.experimental.pallas import tpu as pltpu
from jax.sharding import PartitionSpec as P

OPT_STEP = 4
EPS_SQ = 1e-30
BETA_TWO = 1.0 - OPT_STEP ** -0.8
LR_BASE = min(1e-2, OPT_STEP ** -0.5)

F32 = jnp.float32
MESH = pl.DeviceIdType.MESH
FF, D = 3072.0, 768.0
DIM = 768
THIN = 192
LANES = 128
PAIR = 256
SLABS = 9
PLAIN = 4
WIDE = 6
MATS = 18
STEPS = SLABS
HALF = 384
BLK = 24
ROWCUT = (16, 8)
UP = 2.0 ** 48

HELD = 1
LAG_ADD, LAG_RELAY, LAG_TURN, LAG_RELAY2, LAG_SUM, LAG_DATA, LAG_Z, LAG_MODEL = range(1, 9)


OTHERS = (1, 2, 3)
HALVES = range(2)
THREE = pl.ds(1, 3)
FIRST, SECOND, THIRD = (slice(n, n + 1) for n in range(3))
IN, OUT, QKV, O = slice(4), slice(4, 6), slice(6, 15), slice(15, 18)


def down(v):
    return jnp.sum(v, axis=0, keepdims=True)


def along(v):
    return jnp.sum(v, axis=1, keepdims=True)


def mod4(v):
    return lax.rem(v + 8, 4)


def cut(h, piece):
    return pl.ds(0, ROWCUT[h]) if piece == 0 else pl.ds(ROWCUT[h], BLK - ROWCUT[h])


def slab_of(s):
    if isinstance(s, int):
        return (0, 1, 6, 7, 8, 4, 5, 2, 3)[s]
    return jnp.where(s < 2, s, jnp.where(s < 5, s + 4, jnp.where(s < 7, s - 1, s - 5)))


def kernel(g_in, w_in, r_in, c_in, g_out, w_out, r_out, c_out, g_qkv, w_qkv, r_qkv, c_qkv, g_o, w_o, r_o, c_o,
           w_in_n, r_in_n, c_in_n, w_out_n, r_out_n, c_out_n, w_qkv_n, r_qkv_n, c_qkv_n, w_o_n, r_o_n, c_o_n,
           xin, s0, r0, r1a, r1b, b2, r2a, r2b, grad, gsm, pick_f, pick, vw_in, vw_out, vw_qkv, vw_o,
           vr_in, vc_in, vr_out, vc_out, vr_qkv, vc_qkv, vr_o, vc_o,
           square, thin_a, thin_b, dv_mom, dv_all, dv_own, dv_got, mv_mom, mv_new, mv_own, mv_y, mv_two, mv_z,
           sc_own, sc_got, ld_sem, sm_sem, sent, d2d_r, p1_r, p2_r, dv_r, y_r, z_r, sc_r):
    d = lax.axis_index('data')
    x = lax.axis_index('model')
    core = lax.rem(d, 2)
    y = lax.rem(d // 2, 4)
    z = d // 8

    def at(axis, off, other=0):
        if axis == 'x':
            return {'model': lax.rem(x + off, 4)}
        if axis == 'y':
            return {'data': (z * 4 + lax.rem(y + off, 4)) * 2 + (1 - core if other else core)}
        if axis == 'z':
            return {'data': (lax.rem(z + off, 4) * 4 + y) * 2 + core}
        return {'data': (z * 4 + y) * 2 + (1 - core)}

    def local(src, dst, sem):
        return pltpu.make_async_copy(src, dst, sem)

    loads = [local(g_in.at[k], xin.at[k], ld_sem.at[k]) for k in range(PLAIN)]
    loads += [local(g_out.at[k - PLAIN], xin.at[k], ld_sem.at[k]) for k in range(PLAIN, WIDE)]
    loads += [local(g_qkv.at[pl.ds(DIM * k, DIM)], xin.at[WIDE + k], ld_sem.at[WIDE + k]) for k in HALVES]
    loads += [local(g_qkv.at[pl.ds(2 * DIM, THIN)], xin.at[SLABS - 1, pl.ds(0, THIN)], ld_sem.at[SLABS - 1]),
              local(g_o, xin.at[SLABS - 1, pl.ds(THIN, DIM - THIN)], ld_sem.at[SLABS])]
    small = [(w_in, vw_in), (w_out, vw_out), (w_qkv, vw_qkv), (w_o, vw_o), (r_in, vr_in), (c_in, vc_in),
             (r_out, vr_out), (c_out, vc_out), (r_qkv, vr_qkv), (c_qkv, vc_qkv), (r_o, vr_o), (c_o, vc_o)]
    small = [local(s, t, sm_sem.at[j]) for j, (s, t) in enumerate(small)]
    for cp in [loads[slab_of(j)] for j in range(SLABS)] + loads[SLABS:] + small:
        cp.start()

    barrier = pltpu.get_barrier_semaphore()
    peers = [at('c', 1)] + [at(a, j) for a in 'yzx' for j in OTHERS] + [at('y', j, 1) for j in OTHERS]
    for p in peers:
        pl.semaphore_signal(barrier, inc=1, device_id=p, device_id_type=MESH)
    pl.semaphore_wait(barrier, len(peers))

    def remote(src, dst, ss, rs, dev):
        return pltpu.make_async_remote_copy(src_ref=src, dst_ref=dst, send_sem=ss, recv_sem=rs,
                                            device_id=dev, device_id_type=MESH)

    def d2d(s, h):
        return remote(s0.at[s, h], r0.at[s, h], sent.at[0], d2d_r.at[s, h], at('c', 1))

    def make_pick():
        for side in HALVES:
            cc = (1 - core) if side == 0 else core
            row = lax.broadcasted_iota(jnp.int32, (BLK, HALF), 0)
            col = lax.broadcasted_iota(jnp.int32, (BLK, HALF), 1)
            for b in range(8):
                pick_f[pl.ds(BLK * b, BLK)] = jnp.where(col == row + 2 * BLK * b + BLK * cc, 1.0, 0.0)
            pick[side] = pick_f[...].astype(jnp.bfloat16)

    def part(s, h, side, fn):
        k = slab_of(s)

        def plain():
            first = (core == 0) if side == 1 else (core == 1)
            for g in range(16):
                v = xin[k, pl.ds(2 * BLK * g, 2 * BLK), pl.ds(HALF * h, HALF)].astype(F32)
                fn(pl.ds(g // 4, 1), pl.ds(g % 4, 1), jnp.where(first, v[:BLK], v[BLK:]).reshape(1, 1, BLK, HALF))

        def turned():
            for g in HALVES:
                v = xin[k, pl.ds(HALF * h, HALF), pl.ds(HALF * g, HALF)]
                v = lax.dot_general(pick[side], v, (((1,), (1,)), ((), ())), preferred_element_type=F32)
                fn(pl.ds(2 * g, 2), slice(None), v.reshape(2, 4, BLK, HALF))
        choose(k < PLAIN, plain, turned)

    def choose(cond, yes, no):
        if isinstance(cond, bool):
            return yes() if cond else no()
        pl.when(cond)(yes)
        pl.when(jnp.logical_not(cond))(no)

    def stage_split(s):
        for j in range(SLABS):
            @pl.when(slab_of(s) == j)
            def _(j=j):
                loads[j].wait()
                if j == SLABS - 1:
                    loads[SLABS].wait()
        for h in HALVES:
            def put(zs, ys, v, h=h):
                s0[s, h, zs, ys] = v
            part(s, h, 0, put)
            d2d(s, h).start()

    def ring(h, first):
        axis = ('y', 'z')[h] if first else ('z', 'y')[h]
        return axis, (y if axis == 'y' else z)

    def block(first, s, h, t, piece, flip):
        if not first:
            return b2.at[s, h, t, cut(h ^ flip, piece)]
        return r0.at[s, 0, pl.ds(2 * piece, 2), t] if h == 0 else r0.at[s, 1, t, pl.ds(2 * piece, 2)]

    PLAN = ((-2, 0, 0), (2, 1, 1), (-1, 1, 0), (1, 0, 1), (-1, 0, 0), (1, 1, 1))

    def passing(first, s, h, m, flip):
        _, piece, way = PLAN[m]
        return r1a.at[s, h, way] if first else r2a.at[s, h, way, pl.ds(0, cut(h ^ flip, piece).size)]

    def msg(first, s, h, m, flip):
        axis, n = ring(h, first)
        off, piece, way = PLAN[m]
        recv, landed = (p1_r, r1b) if first else (p2_r, r2b)
        src = block(first, s, h, mod4(n + off), piece, flip)
        if m < 2:
            dst = passing(first, s, h, m, flip)
        else:
            dst = landed.at[s, h, way, pl.ds(2 * piece, 2) if first else cut(h ^ flip, piece)]
        return remote(src, dst, sent.at[1 if first else 2], recv.at[s, h if m < 2 else 2], at(axis, 1 if way else 3))

    def send_raw(first, s, h, flip):
        for m in range(4):
            msg(first, s, h, m, flip).start()

    def wait_for(ref, sem):
        local(ref, ref, sem).wait()

    def stage_add(s):
        for h in HALVES:
            d2d(s, h).wait_recv()

            def add(zs, ys, v, h=h):
                r0[s, h, zs, ys] += v
            part(s, h, 1, add)
            send_raw(True, s, h, 0)

    def relay(first, s, flip):
        for h in HALVES:
            n = ring(h, first)[1]
            wait_for(r1a.at[s, h] if first else b2.at[s, h, 0], (p1_r if first else p2_r).at[s, h])
            for m in HALVES:
                off, piece, _ = PLAN[4 + m]
                ref = block(first, s, h, mod4(n + off), piece, flip)
                ref[...] += passing(first, s, h, m, flip)[...]
                msg(first, s, h, 4 + m, flip).start()

    def stage_turn(s, flip):
        wait_for(r1b.at[s], p1_r.at[s, 2])
        for h in HALVES:
            n = ring(h, True)[1]
            own = r0[s, 0, :, n] if h == 0 else r0[s, 1, n]
            b2[s, h] = own + r1b[s, h, 0] + r1b[s, h, 1]
            send_raw(False, s, h, flip)

    def stage_sum(s):
        wait_for(r2b.at[s], p2_r.at[s, 2])
        for h in HALVES:
            n = ring(h, False)[1]
            grad[slab_of(s), :, pl.ds(HALF * h, HALF)] = (b2[s, h, n] + r2b[s, h, 0] + r2b[s, h, 1]) / 32

    lane = lax.broadcasted_iota(jnp.int32, (1, LANES), 1)
    col = lax.broadcasted_iota(jnp.int32, (1, DIM), 1)
    count = jnp.where(lane < WIDE, FF, D)

    def of_mat(q):
        return jnp.logical_and(col >= THIN * q, col < THIN * q + THIN)

    def total(v):
        return along(down(v))

    def place(j):
        n = 0 if j < 4 else 1 if j < 6 else 2 if j < 15 else 3
        return n, j - (0, 4, 6, 15)[n]

    def weight_of(j):
        n, i = place(j)
        return (vw_in, vw_out, vw_qkv, vw_o)[n][i]

    def prepare():
        for cp in small:
            cp.wait()
        square[...] = jnp.zeros_like(square)
        square[IN, :BLK] = vr_in[...]
        square[OUT, :BLK] = vc_out[...]
        square[QKV, :BLK] = vr_qkv[...]
        square[O, :BLK] = vc_o[...]
        dv_mom[...] = square[...].T[:BLK]
        thin_a[...] = jnp.zeros_like(thin_a)
        thin_a[:9, :THIN] = vc_qkv[...]
        thin_a[9:12, :THIN] = vr_o[...]
        thin_b[...] = pltpu.roll(thin_a[...], 64, 1)
        for k in range(4):
            mv_mom[k] = vc_in[k:k + 1]
        for k in HALVES:
            mv_mom[4 + k] = vr_out[k:k + 1]
        for j in range(12):
            k, q = WIDE + j // 4, j % 4
            if q % 2 == 0:
                mv_mom[k, :, THIN * q:THIN * q + THIN] = thin_a[j:j + 1, :THIN]
            else:
                span = slice(THIN * q - 64, THIN * q + THIN)
                mv_mom[k, :, span] = jnp.where(col[:, :PAIR] < 64, mv_mom[k, :, span], thin_b[j:j + 1])
        mv_own[...] = jnp.zeros_like(mv_own)
        sc_own[...] = jnp.zeros_like(sc_own)
        dv_all[...] = jnp.ones_like(dv_all)
        vec = jnp.zeros((1, LANES), F32)
        for j in range(MATS):
            w = weight_of(j)
            vec = jnp.where(lane == j, total(w * w), vec)
        mv_own[slab_of(SLABS - 1), THIRD, LANES:PAIR] = vec

    def spread(axis, src, dst, ss, rs):
        return [remote(src, dst.at[j], ss, rs, at(axis, j)) for j in OTHERS]

    def start(copies):
        for cp in copies:
            cp.start()

    def rows_of(k):
        return pl.ds(0, 3 if isinstance(k, int) and k == slab_of(SLABS - 1) else 2)

    def dv_copies(k):
        return spread('x', dv_own.at[k], dv_got.at[k], sent.at[3], dv_r.at[k])

    def y_copies(k):
        src = mv_own.at[k, rows_of(k)]
        return [remote(src, mv_y.at[k, j + 4 * other, rows_of(k)], sent.at[4 + rows_of(k).size], y_r.at[k],
                       at('y', j, other) if j else at('c', 1)) for j in range(4) for other in HALVES if j or other]

    def z_copies(k):
        return [remote(mv_two.at[k, rows_of(k)], mv_z.at[k, j, rows_of(k)], sent.at[6 + rows_of(k).size], z_r.at[k], at('z', j))
                for j in OTHERS]

    def sums(k):
        g = grad[k]
        s = g * g + EPS_SQ
        mv_own[k, FIRST] = down(s)

        def wide():
            dv_own[k] = jnp.where(lane == k, along(s), 0.0)

        def thin():
            dv = jnp.zeros((BLK, LANES), F32)
            for q in range(4):
                dv = jnp.where(lane == 4 * k - 18 + q, along(jnp.where(of_mat(q), s, 0.0)), dv)
            dv_own[k] = dv
        choose(k < WIDE, wide, thin)
        start(dv_copies(k))

    def mats_of(k):
        low = jnp.where(k < WIDE, k, 4 * k - 18)
        return jnp.logical_and(lane >= low, lane < jnp.where(k < WIDE, k + 1, 4 * k - 14))

    def data_side(k):
        mine = mats_of(k)
        wait_for(dv_got.at[k, THREE], dv_r.at[k])
        got = (dv_own[k] + dv_got[k, 2]) + (dv_got[k, 1] + dv_got[k, 3])
        new = BETA_TWO * dv_mom[...] + (1.0 - BETA_TWO) * (got / count)
        dv_all[...] = jnp.where(mine, new, dv_all[...])
        if rows_of(k).size == 3:
            mv_own[k, THIRD, :LANES] = down(dv_all[...])
        inv = 1.0 / jnp.sqrt(jnp.where(mine, new, 1.0))

        def column(j):
            return along(jnp.where(lane == j, inv, 0.0))

        def scaled(factor):
            q = grad[k] * factor
            grad[k] = q
            q = q * UP
            mv_own[k, SECOND] = down(q * q)

        def wide():
            scaled(column(k))

        def thin():
            factor = column(4 * k - 15)
            for q in (2, 1, 0):
                factor = jnp.where(col < THIN * q + THIN, column(4 * k - 18 + q), factor)
            scaled(factor)
        choose(k < WIDE, wide, thin)
        start(y_copies(k))

    def stage_z(k):
        wait_for(mv_y.at[k, pl.ds(1, 7), rows_of(k)], y_r.at[k])
        one = [mv_own[k] + mv_y[k, 4]] + [mv_y[k, j] + mv_y[k, 4 + j] for j in OTHERS]
        mv_two[k] = (one[0] + one[2]) + (one[1] + one[3])
        start(z_copies(k))

    def model_side(k):
        mine = mats_of(k)
        wait_for(mv_z.at[k, THREE, rows_of(k)], z_r.at[k])
        v = (mv_two[k] + mv_z[k, 2]) + (mv_z[k, 1] + mv_z[k, 3])
        new = BETA_TWO * mv_mom[k] + (1.0 - BETA_TWO) * (v[FIRST] / D)
        mv_new[k] = new
        inv = 1.0 / jnp.sqrt(new)
        a = jnp.sqrt(v[SECOND]) * inv * (1.0 / UP)
        a = a * a
        u = grad[k] * inv

        def wide():
            sc_own[FIRST] = jnp.where(mine, total(a), sc_own[FIRST])
            sc_own[SECOND] = jnp.where(mine, total(new), sc_own[SECOND])
            grad[k] = u

        def thin():
            upd, row = sc_own[FIRST], sc_own[SECOND]
            for q in range(4):
                j = 4 * k - 18 + q
                upd = jnp.where(lane == j, total(jnp.where(of_mat(q), a, 0.0)), upd)
                row = jnp.where(lane == j, total(jnp.where(of_mat(q), new, 0.0)), row)
                if q % 2 == 0:
                    gsm[j - WIDE] = u[:, THIN * q:THIN * q + THIN]
                else:
                    gsm[j - WIDE] = pltpu.roll(u[:, THIN * q - 64:THIN * q + THIN], THIN, 1)[:, :THIN]
            sc_own[FIRST] = upd
            sc_own[SECOND] = row
        choose(k < WIDE, wide, thin)
        if rows_of(k).size == 3:
            by_model = jnp.logical_or(jnp.logical_and(lane >= 4, lane < 6), lane >= 15)
            sc_own[SECOND] = jnp.where(by_model, sc_own[SECOND], v[THIRD, :LANES] / 4)
            sc_own[THIRD] = v[THIRD, LANES:PAIR]

    def by_parity(fn):
        def stage(s):
            choose(lax.rem(s, 2) == 0, lambda: fn(s, 0), lambda: fn(s, 1))
        return stage

    def turn(s):
        stage_turn(s, s % 2)

    def relay2(s):
        relay(False, s, s % 2)

    def finish(s):
        stage_sum(s)
        sums(slab_of(s))

    def relay1(s):
        relay(True, s, 0)

    def data(s):
        data_side(slab_of(s))

    def to_z(s):
        stage_z(slab_of(s))

    def model(s):
        model_side(slab_of(s))

    early = ((0, stage_split), (LAG_ADD, stage_add), (LAG_RELAY, relay1))
    late = ((LAG_TURN, by_parity(stage_turn)), (LAG_RELAY2, by_parity(lambda s, flip: relay(False, s, flip))),
            (LAG_SUM, finish), (LAG_DATA, data), (LAG_Z, to_z), (LAG_MODEL, model))

    def trip(i, carry):
        for lag, stage in early:
            @pl.when(i >= lag)
            def _(lag=lag, stage=stage):
                stage(i - lag)

        @pl.when(i == 1)
        def _():
            make_pick()
        for lag, stage in late:
            @pl.when(jnp.logical_and(i >= lag, i < HELD + lag))
            def _(lag=lag, stage=stage):
                stage(i - lag)

        @pl.when(i == LAG_TURN)
        def _():
            prepare()
        return carry
    lax.fori_loop(0, STEPS, trip, 0)

    last = STEPS - 1
    mids = range(HELD, last - 1)
    held = range(HELD, last)

    def rest(i):
        for lag, stage in ((LAG_TURN, turn), (LAG_RELAY2, relay2), (LAG_SUM, finish), (LAG_DATA, data), (LAG_Z, to_z),
                           (LAG_MODEL, model)):
            if 0 <= i - lag < HELD:
                stage(i - lag)

    def each(stage, steps):
        for s in steps:
            stage(s)
    stage_add(last)
    relay1(last - 1)
    relay1(last)
    each(turn, mids)
    rest(STEPS)
    turn(last - 1)
    turn(last)
    each(relay2, mids)
    rest(STEPS + 1)
    relay2(last - 1)
    relay2(last)
    rest(STEPS + 2)
    each(finish, mids)
    finish(last - 1)
    rest(STEPS + 3)
    finish(last)
    rest(STEPS + 4)
    each(data, held)
    data(last)
    each(to_z, held)
    to_z(last)
    each(model, held)
    model(last)

    sc_cp = spread('x', sc_own, sc_got, sent.at[SLABS + 1], sc_r.at[0])
    start(sc_cp)

    square[:BLK] = dv_all[...]
    turned = square[...].T
    r_in_n[...] = turned[IN, :BLK]
    c_out_n[...] = turned[OUT, :BLK]
    r_qkv_n[...] = turned[QKV, :BLK]
    c_o_n[...] = turned[O, :BLK]
    for k in range(4):
        c_in_n[k:k + 1] = mv_new[k]
    for k in HALVES:
        r_out_n[k:k + 1] = mv_new[4 + k]
    for j in range(12):
        k, q = WIDE + j // 4, j % 4
        if q % 2 == 0:
            thin_a[j:j + 1, :THIN] = mv_new[k, :, THIN * q:THIN * q + THIN]
        else:
            thin_b[j:j + 1] = mv_new[k, :, THIN * q - 64:THIN * q + THIN]
    odd = lax.rem(lax.broadcasted_iota(jnp.int32, thin_a.shape, 0), 2) == 1
    thin_a[...] = jnp.where(odd, pltpu.roll(thin_b[...], THIN, 1), thin_a[...])
    c_qkv_n[...] = thin_a[:9, :THIN]
    r_o_n[...] = thin_a[9:12, :THIN]

    few = STEPS - 1
    for j, ref in enumerate((s0, s0.at[:, :, pl.ds(0, 3)], b2.at[:, :, pl.ds(0, 3)], dv_got.at[:, pl.ds(0, 3)])):
        wait_for(ref, sent.at[j])
    wait_for(mv_y.at[pl.ds(0, few), pl.ds(1, 7), pl.ds(0, 2)], sent.at[6])
    wait_for(mv_y.at[0, pl.ds(1, 7), pl.ds(0, 3)], sent.at[7])
    wait_for(mv_z.at[pl.ds(0, few), THREE, pl.ds(0, 2)], sent.at[8])
    wait_for(mv_z.at[0, THREE, pl.ds(0, 3)], sent.at[9])

    wait_for(sc_got.at[THREE], sc_r.at[0])
    sc = (sc_own[...] + sc_got[2]) + (sc_got[1] + sc_got[3])
    full = jnp.where(lane < WIDE, FF * D, D * D)
    rows = jnp.where(jnp.logical_and(lane >= 4, lane < 6), FF, D)
    row_mean = sc[SECOND] / rows
    upd_rms = jnp.sqrt(row_mean * (sc[FIRST] / full))
    w_rms = jnp.sqrt(sc[THIRD] / full)
    scale = LR_BASE * jnp.maximum(1e-3, w_rms) * (jnp.sqrt(row_mean) / jnp.maximum(1.0, upd_rms))
    for j in range(MATS):
        upd = grad[j] if j < WIDE else gsm[j - WIDE]
        new = weight_of(j) - scale[:, j:j + 1] * upd
        n, i = place(j)
        (w_in_n, w_out_n, w_qkv_n, w_o_n)[n][i] = new
    wait_for(sc_got.at[THREE], sent.at[SLABS + 1])


def write_out(*refs):
    n = len(refs) // 2
    copies = [pltpu.make_async_copy(refs[j], refs[n + j], refs[-1].at[j]) for j in range(n)]
    for cp in copies:
        cp.start()
    for cp in copies:
        cp.wait()


def solution(mesh):
    rows_data = (P('data', None, None, 'model'), P(None, 'data', 'model'), P(None, 'data'), P(None, 'model'))
    rows_model = (P('data', None, 'model', None), P(None, 'model', 'data'), P(None, 'model'), P(None, 'data'))
    DMA = pltpu.SemaphoreType.DMA

    def step_all(grad_in, w_in, row_in, col_in, grad_out, w_out, row_out, col_out,
                 grad_qkv, w_qkv, row_qkv, col_qkv, grad_o, w_o, row_o, col_o):
        args = (grad_in[0], w_in, row_in, col_in,
                grad_out[0], w_out.swapaxes(1, 2), row_out, col_out,
                grad_qkv[0].swapaxes(1, 2).reshape(-1, DIM), w_qkv, row_qkv, col_qkv,
                grad_o[0].reshape(-1, DIM), w_o.swapaxes(1, 2), row_o, col_o)
        small = [a for n, a in enumerate(args) if n % 4]
        outs = [jax.ShapeDtypeStruct(a.shape, a.dtype) for a in small]
        held = [pltpu.VMEM(a.shape, a.dtype) for a in small]
        vm = lambda *s: pltpu.VMEM(s, F32)
        res = pl.pallas_call(
            kernel,
            out_shape=held,
            in_specs=[pl.BlockSpec(memory_space=pl.ANY)] * len(args),
            out_specs=[pl.BlockSpec(memory_space=pltpu.VMEM)] * len(outs),
            scratch_shapes=[
                pltpu.VMEM((SLABS, DIM, DIM), jnp.bfloat16),
                vm(STEPS, 2, 4, 4, BLK, HALF), vm(STEPS, 2, 4, 4, BLK, HALF),
                vm(STEPS, 2, 2, 2, BLK, HALF), vm(STEPS, 2, 2, 4, BLK, HALF), vm(STEPS, 2, 4, BLK, HALF),
                vm(STEPS, 2, 2, 16, HALF), vm(STEPS, 2, 2, BLK, HALF),
                vm(SLABS, BLK, DIM), vm(12, BLK, THIN),
                vm(THIN, HALF), pltpu.VMEM((2, THIN, HALF), jnp.bfloat16)]
            + [vm(*a.shape) for n, a in enumerate(small) if n % 3 == 0] + [vm(*a.shape) for n, a in enumerate(small) if n % 3]
            + [vm(LANES, LANES), vm(16, PAIR), vm(16, PAIR), vm(BLK, LANES), vm(BLK, LANES),
               vm(SLABS, BLK, LANES), vm(SLABS, 4, BLK, LANES), vm(SLABS, 1, DIM), vm(SLABS, 1, DIM),
               vm(SLABS, 4, DIM), vm(SLABS, 8, 4, DIM), vm(SLABS, 4, DIM), vm(SLABS, 4, 4, DIM), vm(8, LANES), vm(4, 8, LANES),
               DMA((SLABS + 1,)), DMA((len(small),)), DMA((SLABS + 2,)), DMA((STEPS, 2)), DMA((STEPS, 3)), DMA((STEPS, 3)),
               DMA((SLABS,)), DMA((SLABS,)), DMA((SLABS,)), DMA((1,))],
            compiler_params=pltpu.CompilerParams(
                collective_id=0, has_side_effects=True, vmem_limit_bytes=58_000_000),
            name='adafactor',
        )(*args)
        res = list(pl.pallas_call(
            write_out,
            out_shape=outs,
            in_specs=[pl.BlockSpec(memory_space=pltpu.VMEM)] * len(outs),
            out_specs=[pl.BlockSpec(memory_space=pl.ANY)] * len(outs),
            scratch_shapes=[DMA((len(outs),))],
            name='write_out',
        )(*[pltpu.with_memory_space_constraint(r, pltpu.VMEM) for r in res]))
        for n in (3, SLABS):
            res[n] = res[n].swapaxes(1, 2)
        return tuple(res)

    in_specs = rows_data + rows_model + rows_data + rows_model
    out_specs = rows_data[1:] + rows_model[1:] + rows_data[1:] + rows_model[1:]
    return jax.shard_map(step_all, mesh=mesh, in_specs=in_specs, out_specs=out_specs, check_vma=False)
```

```python
import jax
import jax.numpy as jnp
from jax import lax
from jax.experimental import pallas as pl
from jax.experimental.pallas import tpu as pltpu
from jax.sharding import PartitionSpec as P

OPT_STEP = 4
EPS_SQ = 1e-30
BETA_TWO = 1.0 - OPT_STEP ** -0.8
LR_BASE = min(1e-2, OPT_STEP ** -0.5)

F32 = jnp.float32
MESH = pl.DeviceIdType.MESH
FF, D = 3072.0, 768.0
DIM = 768
THIN = 192
LANES = 128
PAIR = 256
SLABS = 9
PLAIN = 4
WIDE = 6
MATS = 18
STEPS = SLABS
HALF = 384
BLK = 24
ROWCUT = (16, 8)
UP = 2.0 ** 48

GROUPS = tuple(range(n, min(n + 2, STEPS)) for n in range(0, STEPS, 2))
PARTS = 3


OTHERS = (1, 2, 3)
HALVES = range(2)
THREE, SEVEN = pl.ds(1, 3), pl.ds(1, 7)
DUO, TRIO = pl.ds(0, 2), pl.ds(0, 3)
FIRST, SECOND, THIRD, FOURTH = (slice(n, n + 1) for n in range(4))
IN, OUT, QKV, O = slice(4), slice(4, 6), slice(6, 15), slice(15, 18)


def down(v):
    return jnp.sum(v, axis=0, keepdims=True)


def along(v):
    return jnp.sum(v, axis=1, keepdims=True)


def mod4(v):
    return lax.rem(v + 8, 4)


def span(h, c):
    return pl.ds(HALF * h + LANES * c, LANES)


def cut(h, piece):
    return pl.ds(0, ROWCUT[h]) if piece == 0 else pl.ds(ROWCUT[h], BLK - ROWCUT[h])


def slab_of(s):
    if isinstance(s, int):
        return (0, 1, 6, 7, 8, 4, 5, 2, 3)[s]
    return jnp.where(s < 2, s, jnp.where(s < 5, s + 4, jnp.where(s < 7, s - 1, s - 5)))


def kernel(g_in, w_in, r_in, c_in, g_out, w_out, r_out, c_out, g_qkv, w_qkv, r_qkv, c_qkv, g_o, w_o, r_o, c_o,
           w_in_n, r_in_n, c_in_n, w_out_n, r_out_n, c_out_n, w_qkv_n, r_qkv_n, c_qkv_n, w_o_n, r_o_n, c_o_n,
           xin, s0, r0, r1a, r1b, b2, r2a, r2b, grad, gsm, pick_f, pick, vw_in, vw_out, vw_qkv, vw_o,
           vr_in, vc_in, vr_out, vc_out, vr_qkv, vc_qkv, vr_o, vc_o,
           square, thin_a, thin_b, dv_mom, dv_all, dv_own, dv_got, mv_mom, mv_new, mv_own, mv_y, mv_two, mv_z,
           sc_own, sc_got, ld_sem, sm_sem, sent, first_r, d2d_r, passed, whole, dv_r, sc_r):
    d = lax.axis_index('data')
    x = lax.axis_index('model')
    core = lax.rem(d, 2)
    y = lax.rem(d // 2, 4)
    z = d // 8

    def at(axis, off, other=0):
        if axis == 'x':
            return {'model': lax.rem(x + off, 4)}
        if axis == 'y':
            return {'data': (z * 4 + lax.rem(y + off, 4)) * 2 + (1 - core if other else core)}
        if axis == 'z':
            return {'data': (lax.rem(z + off, 4) * 4 + y) * 2 + core}
        return {'data': (z * 4 + y) * 2 + (1 - core)}

    def local(src, dst, sem):
        return pltpu.make_async_copy(src, dst, sem)

    loads = [None] + [local(g_in.at[k], xin.at[k], ld_sem.at[k]) for k in range(1, PLAIN)]
    loads += [local(g_out.at[k - PLAIN], xin.at[k], ld_sem.at[k]) for k in range(PLAIN, WIDE)]
    loads += [local(g_qkv.at[pl.ds(DIM * k, DIM)], xin.at[WIDE + k], ld_sem.at[WIDE + k]) for k in HALVES]
    loads += [local(g_qkv.at[pl.ds(2 * DIM, THIN)], xin.at[SLABS - 1, pl.ds(0, THIN)], ld_sem.at[SLABS - 1]),
              local(g_o, xin.at[SLABS - 1, pl.ds(THIN, DIM - THIN)], ld_sem.at[SLABS])]
    small = [(w_in, vw_in), (w_out, vw_out), (w_qkv, vw_qkv), (w_o, vw_o), (r_in, vr_in), (c_in, vc_in),
             (r_out, vr_out), (c_out, vc_out), (r_qkv, vr_qkv), (c_qkv, vc_qkv), (r_o, vr_o), (c_o, vc_o)]
    small = [local(s, t, sm_sem.at[j]) for j, (s, t) in enumerate(small)]
    loads[0] = [local(g_in.at[0, :, span(h, c)], xin.at[0, :, span(h, c)], ld_sem.at[SLABS + 1 + h + 2 * c])
                for c in range(PARTS) for h in HALVES]
    for cp in loads[0] + [loads[1]]:
        cp.start()

    barrier = pltpu.get_barrier_semaphore()
    peers = [at('c', 1)] + [at(a, j) for a in 'yzx' for j in OTHERS] + [at('y', j, 1) for j in OTHERS]
    for p in peers:
        pl.semaphore_signal(barrier, inc=1, device_id=p, device_id_type=MESH)

    def remote(src, dst, ss, rs, dev):
        return pltpu.make_async_remote_copy(src_ref=src, dst_ref=dst, send_sem=ss, recv_sem=rs,
                                            device_id=dev, device_id_type=MESH)

    def d2d(s, h):
        return remote(s0.at[s, h], r0.at[s, h], sent.at[0], d2d_r.at[s], at('c', 1))

    def make_pick():
        for side in HALVES:
            cc = (1 - core) if side == 0 else core
            row = lax.broadcasted_iota(jnp.int32, (BLK, HALF), 0)
            col = lax.broadcasted_iota(jnp.int32, (BLK, HALF), 1)
            for b in range(8):
                pick_f[pl.ds(BLK * b, BLK)] = jnp.where(col == row + 2 * BLK * b + BLK * cc, 1.0, 0.0)
            pick[side] = pick_f[...].astype(jnp.bfloat16)

    def part(s, h, side, fn, cols=None):
        k = slab_of(s)

        def plain():
            first = (core == 0) if side == 1 else (core == 1)
            for g in range(16):
                v = xin[k, pl.ds(2 * BLK * g, 2 * BLK), cols or pl.ds(HALF * h, HALF)].astype(F32)
                fn(pl.ds(g // 4, 1), pl.ds(g % 4, 1), jnp.where(first, v[:BLK], v[BLK:]).reshape(1, 1, BLK, -1))

        def turned():
            for g in HALVES:
                v = xin[k, pl.ds(HALF * h, HALF), pl.ds(HALF * g, HALF)]
                v = lax.dot_general(pick[side], v, (((1,), (1,)), ((), ())), preferred_element_type=F32)
                fn(pl.ds(2 * g, 2), slice(None), v.reshape(2, 4, BLK, HALF))
        choose(k < PLAIN, plain, turned)

    def choose(cond, yes, no):
        if isinstance(cond, bool):
            return yes() if cond else no()
        pl.when(cond)(yes)
        pl.when(jnp.logical_not(cond))(no)

    def stage_split(s):
        for j in range(1, SLABS):
            @pl.when(slab_of(s) == j)
            def _(j=j):
                loads[j].wait()
                if j == SLABS - 1:
                    loads[SLABS].wait()
        for h in HALVES:
            split_half(s, h)
            d2d(s, h).start()

    def split_half(s, h):
        def put(zs, ys, v):
            s0[s, h, zs, ys] = v
        part(s, h, 0, put)

    def first_d2d(h, c):
        cols = span(0, c)
        return remote(s0.at[0, h, :, :, :, cols], r0.at[0, h, :, :, :, cols], sent.at[0], first_r.at[h, c], at('c', 1))

    def ring(h, first):
        axis = ('y', 'z')[h] if first else ('z', 'y')[h]
        return axis, (y if axis == 'y' else z)

    def block(first, s, h, t, piece, flip):
        if not first:
            return b2.at[s, h, t, cut(h ^ flip, piece)]
        return r0.at[s, 0, pl.ds(2 * piece, 2), t] if h == 0 else r0.at[s, 1, t, pl.ds(2 * piece, 2)]

    PLAN = ((-2, 0, 0), (2, 1, 1), (-1, 1, 0), (1, 0, 1), (-1, 0, 0), (1, 1, 1))

    def passing(first, s, h, m, flip):
        _, piece, way = PLAN[m]
        return r1a.at[s, h, way] if first else r2a.at[s, h, way, pl.ds(0, cut(h ^ flip, piece).size)]

    def msg(first, s, h, m, flip, cols=slice(None)):
        axis, n = ring(h, first)
        off, piece, way = PLAN[m]
        landed = r1b if first else r2b
        src = block(first, s, h, mod4(n + off), piece, flip)
        if m < 2:
            dst = passing(first, s, h, m, flip)
        else:
            dst = landed.at[s, h, way, pl.ds(2 * piece, 2) if first else cut(h ^ flip, piece)]
        if first:
            src, dst = src.at[:, :, cols], dst.at[:, :, cols]
        return remote(src, dst, sent.at[1 if first else 2], passed.at[s] if m < 2 else whole.at[s] if first else d2d_r.at[s], at(axis, 1 if way else 3))

    def send_raw(first, s, h, flip, cols=slice(None)):
        for m in range(4):
            msg(first, s, h, m, flip, cols).start()

    def wait_for(ref, sem):
        local(ref, ref, sem).wait()

    def stage_add(s):
        wait_for(r0.at[s], d2d_r.at[s])
        for h in HALVES:

            def add(zs, ys, v, h=h):
                r0[s, h, zs, ys] += v
            part(s, h, 1, add)
            send_raw(True, s, h, 0)

    def first_split():
        for c in range(PARTS):
            for h in HALVES:
                def put(zs, ys, v, h=h, c=c):
                    s0[0, h, zs, ys, :, span(0, c)] = v
                loads[0][h + 2 * c].wait()
                part(0, h, 0, put, span(h, c))
                if h == 0 and c == 0:
                    pl.semaphore_wait(barrier, len(peers))
                first_d2d(h, c).start()

    def first_add():
        for c in range(PARTS):
            for h in HALVES:
                def add(zs, ys, v, h=h, c=c):
                    r0[0, h, zs, ys, :, span(0, c)] += v
                first_d2d(h, c).wait_recv()
                part(0, h, 1, add, span(h, c))
                send_raw(True, 0, h, 0, span(0, c))

    def relay(first, s, flip):
        wait_for(r1a.at[s] if first else b2.at[s, 0, DUO], passed.at[s])
        for h in HALVES:
            n = ring(h, first)[1]
            for m in HALVES:
                off, piece, _ = PLAN[4 + m]
                ref = block(first, s, h, mod4(n + off), piece, flip)
                ref[...] += passing(first, s, h, m, flip)[...]
                msg(first, s, h, 4 + m, flip).start()

    def stage_turn(s, flip):
        wait_for(r1b.at[s], whole.at[s])
        for h in HALVES:
            n = ring(h, True)[1]
            own = r0[s, 0, :, n] if h == 0 else r0[s, 1, n]
            b2[s, h] = own + r1b[s, h, 0] + r1b[s, h, 1]
            send_raw(False, s, h, flip)

    def stage_sum(s):
        wait_for(r2b.at[s], d2d_r.at[s])
        for h in HALVES:
            n = ring(h, False)[1]
            grad[slab_of(s), :, pl.ds(HALF * h, HALF)] = (b2[s, h, n] + r2b[s, h, 0] + r2b[s, h, 1]) / 32

    lane = lax.broadcasted_iota(jnp.int32, (1, LANES), 1)
    col = lax.broadcasted_iota(jnp.int32, (1, DIM), 1)
    count = jnp.where(lane < WIDE, FF, D)

    def of_mat(q):
        return jnp.logical_and(col >= THIN * q, col < THIN * q + THIN)

    def total(v):
        return along(down(v))

    def place(j):
        n = 0 if j < 4 else 1 if j < 6 else 2 if j < 15 else 3
        return n, j - (0, 4, 6, 15)[n]

    def weight_of(j):
        n, i = place(j)
        return (vw_in, vw_out, vw_qkv, vw_o)[n][i]

    def prepare():
        for cp in small:
            cp.wait()
        square[...] = jnp.zeros_like(square)
        square[IN, :BLK] = vr_in[...]
        square[OUT, :BLK] = vc_out[...]
        square[QKV, :BLK] = vr_qkv[...]
        square[O, :BLK] = vc_o[...]
        dv_mom[...] = square[...].T[:BLK]
        thin_a[...] = jnp.zeros_like(thin_a)
        thin_a[:9, :THIN] = vc_qkv[...]
        thin_a[9:12, :THIN] = vr_o[...]
        thin_b[...] = pltpu.roll(thin_a[...], 64, 1)
        for k in range(4):
            mv_mom[k] = vc_in[k:k + 1]
        for k in HALVES:
            mv_mom[4 + k] = vr_out[k:k + 1]
        for j in range(12):
            k, q = WIDE + j // 4, j % 4
            if q % 2 == 0:
                mv_mom[k, :, THIN * q:THIN * q + THIN] = thin_a[j:j + 1, :THIN]
            else:
                span = slice(THIN * q - 64, THIN * q + THIN)
                mv_mom[k, :, span] = jnp.where(col[:, :PAIR] < 64, mv_mom[k, :, span], thin_b[j:j + 1])
        mv_own[...] = jnp.zeros_like(mv_own)
        sc_own[...] = jnp.zeros_like(sc_own)
        dv_all[...] = jnp.ones_like(dv_all)
        vec = jnp.zeros((1, LANES), F32)
        for j in range(MATS):
            w = weight_of(j)
            vec = jnp.where(lane == j, total(w * w), vec)
        mv_own[slab_of(0), THIRD, LANES:PAIR] = vec
        mv_own[slab_of(0), THIRD, :LANES] = down(dv_mom[...])

    def spread(axis, src, dst, ss, rs):
        return [remote(src, dst.at[j], ss, rs, at(axis, j)) for j in OTHERS]

    def start(copies):
        for cp in copies:
            cp.start()

    def rows_of(k):
        return pl.ds(0, 3 if k == slab_of(0) else 2)

    def dv_copies(n):
        return spread('x', dv_own.at[n], dv_got.at[n], sent.at[3], dv_r.at[n])

    def y_copies(k):
        src = mv_own.at[k, rows_of(k)]
        return [remote(src, mv_y.at[k, j + 4 * other, rows_of(k)], sent.at[4 + rows_of(k).size], ld_sem.at[k],
                       at('y', j, other) if j else at('c', 1)) for j in range(4) for other in HALVES if j or other]

    def z_copies(k):
        return [remote(mv_two.at[k, rows_of(k)], mv_z.at[k, j, rows_of(k)], sent.at[6 + rows_of(k).size], whole.at[k], at('z', j))
                for j in OTHERS]

    def sums(k):
        g = grad[k]
        s = g * g + EPS_SQ
        mv_own[k, FIRST] = down(s)
        if k < WIDE:
            return jnp.where(lane == k, along(s), 0.0)
        dv = jnp.zeros((BLK, LANES), F32)
        for q in range(4):
            low = HALF * (q // 2)
            t = jnp.where(of_mat(q)[:, low:low + HALF], s[:, low:low + HALF], 0.0)
            dv = jnp.where(lane == 4 * k - 18 + q, along(t), dv)
        return dv

    def mats_of(k):
        low, high = (k, k + 1) if k < WIDE else (4 * k - 18, 4 * k - 14)
        return jnp.logical_and(lane >= low, lane < high)

    def finish(n):
        dv = jnp.zeros((BLK, LANES), F32)
        for s in GROUPS[n]:
            stage_sum(s)
            dv = dv + sums(slab_of(s))
        dv_own[n] = dv
        start(dv_copies(n))

    def data(n):
        wait_for(dv_got.at[n, THREE], dv_r.at[n])
        got = (dv_own[n] + dv_got[n, 2]) + (dv_got[n, 1] + dv_got[n, 3])
        new = BETA_TWO * dv_mom[...] + (1.0 - BETA_TWO) * (got / count)
        mine = lane < 0
        for s in GROUPS[n]:
            mine = jnp.logical_or(mine, mats_of(slab_of(s)))
        dv_all[...] = jnp.where(mine, new, dv_all[...])
        inv = 1.0 / jnp.sqrt(jnp.where(mine, new, 1.0))
        for s in GROUPS[n]:
            k = slab_of(s)
            if k < WIDE:
                factor = inv[:, k:k + 1]
            else:
                factor = inv[:, 4 * k - 15:4 * k - 14]
                for q in reversed(range(3)):
                    factor = jnp.where(col < THIN * q + THIN, inv[:, 4 * k - 18 + q:4 * k - 17 + q], factor)
            g = grad[k] * factor
            grad[k] = g
            g = g * UP
            mv_own[k, SECOND] = down(g * g)
            start(y_copies(k))

    def stage_z(k):
        wait_for(mv_y.at[k, SEVEN, rows_of(k)], ld_sem.at[k])
        one = [mv_own[k] + mv_y[k, 4]] + [mv_y[k, j] + mv_y[k, 4 + j] for j in OTHERS]
        mv_two[k] = (one[0] + one[2]) + (one[1] + one[3])
        start(z_copies(k))

    def model_side(k):
        mine = mats_of(k)
        wait_for(mv_z.at[k, THREE, rows_of(k)], whole.at[k])
        v = (mv_two[k] + mv_z[k, 2]) + (mv_z[k, 1] + mv_z[k, 3])
        new = BETA_TWO * mv_mom[k] + (1.0 - BETA_TWO) * (v[FIRST] / D)
        mv_new[k] = new
        inv = 1.0 / jnp.sqrt(new)
        a = jnp.sqrt(v[SECOND]) * inv * (1.0 / UP)
        a = a * a
        u = grad[k] * inv

        by_data = (1.0 - BETA_TWO) * (v[FIRST] / (FF if k < WIDE else D))

        def wide():
            sc_own[FIRST] = jnp.where(mine, total(a), sc_own[FIRST])
            sc_own[SECOND] = jnp.where(mine, total(by_data if k < 4 else new), sc_own[SECOND])
            grad[k] = u

        def thin():
            upd, row = sc_own[FIRST], sc_own[SECOND]
            for q in range(4):
                j = 4 * k - 18 + q
                upd = jnp.where(lane == j, total(jnp.where(of_mat(q), a, 0.0)), upd)
                row = jnp.where(lane == j, total(jnp.where(of_mat(q), by_data if j < 15 else new, 0.0)), row)
                if q % 2 == 0:
                    gsm[j - WIDE] = u[:, THIN * q:THIN * q + THIN]
                else:
                    gsm[j - WIDE] = pltpu.roll(u[:, THIN * q - 64:THIN * q + THIN], THIN, 1)[:, :THIN]
            sc_own[FIRST] = upd
            sc_own[SECOND] = row
        choose(k < WIDE, wide, thin)
        if rows_of(k).size == 3:
            sc_own[THIRD] = v[THIRD, LANES:PAIR]
            sc_own[FOURTH] = v[THIRD, :LANES]

    def turn(s):
        stage_turn(s, s % 2)

    def relay2(s):
        relay(False, s, s % 2)

    def relay1(s):
        relay(True, s, 0)

    def to_z(s):
        stage_z(slab_of(s))

    def model(s):
        model_side(slab_of(s))

    first_split()
    for cp in [loads[slab_of(j)] for j in range(2, SLABS)] + loads[SLABS:] + small:
        cp.start()
    first_add()

    def trip(i, carry):
        @pl.when(i > 1)
        def _():
            stage_add(i - 1)
        stage_split(i)

        @pl.when(i > 1)
        def _():
            relay1(i - 2)

        @pl.when(i == 1)
        def _():
            make_pick()

        @pl.when(i == 3)
        def _():
            prepare()
        return carry
    lax.fori_loop(1, STEPS, trip, 0)

    def each(stage, steps):
        for s in steps:
            stage(s)

    last = STEPS - 1
    stage_add(last)
    relay1(last - 1)
    relay1(last)
    for stage in (turn, relay2):
        each(stage, range(STEPS))
    for stage in (finish, data):
        each(stage, range(len(GROUPS)))
    for stage in (to_z, model):
        each(stage, range(STEPS))

    sc_cp = spread('x', sc_own, sc_got, sent.at[SLABS + 1], sc_r.at[0])
    start(sc_cp)

    square[:BLK] = dv_all[...]
    turned = square[...].T
    r_in_n[...] = turned[IN, :BLK]
    c_out_n[...] = turned[OUT, :BLK]
    r_qkv_n[...] = turned[QKV, :BLK]
    c_o_n[...] = turned[O, :BLK]
    for k in range(4):
        c_in_n[k:k + 1] = mv_new[k]
    for k in HALVES:
        r_out_n[k:k + 1] = mv_new[4 + k]
    for j in range(12):
        k, q = WIDE + j // 4, j % 4
        if q % 2 == 0:
            thin_a[j:j + 1, :THIN] = mv_new[k, :, THIN * q:THIN * q + THIN]
        else:
            thin_b[j:j + 1] = mv_new[k, :, THIN * q - 64:THIN * q + THIN]
    odd = lax.rem(lax.broadcasted_iota(jnp.int32, thin_a.shape, 0), 2) == 1
    thin_a[...] = jnp.where(odd, pltpu.roll(thin_b[...], THIN, 1), thin_a[...])
    c_qkv_n[...] = thin_a[:9, :THIN]
    r_o_n[...] = thin_a[9:12, :THIN]

    few = STEPS - 1
    for j, ref in enumerate((s0, s0.at[:, :, TRIO], b2.at[:, :, TRIO], dv_got.at[:, TRIO])):
        wait_for(ref, sent.at[j])
    wait_for(mv_y.at[pl.ds(0, few), SEVEN, DUO], sent.at[6])
    wait_for(mv_y.at[0, SEVEN, TRIO], sent.at[7])
    wait_for(mv_z.at[pl.ds(0, few), THREE, DUO], sent.at[8])
    wait_for(mv_z.at[0, THREE, TRIO], sent.at[9])

    wait_for(sc_got.at[THREE], sc_r.at[0])
    sc = (sc_own[...] + sc_got[2]) + (sc_got[1] + sc_got[3])
    full = jnp.where(lane < WIDE, FF * D, D * D)
    rows = jnp.where(jnp.logical_and(lane >= 4, lane < 6), FF, D)
    by_model = jnp.logical_or(jnp.logical_and(lane >= 4, lane < 6), lane >= 15)
    row_mean = (sc[SECOND] + jnp.where(by_model, 0.0, BETA_TWO * (sc[FOURTH] / 4))) / rows
    upd_rms = jnp.sqrt(row_mean * (sc[FIRST] / full))
    w_rms = jnp.sqrt(sc[THIRD] / full)
    scale = LR_BASE * jnp.maximum(1e-3, w_rms) * (jnp.sqrt(row_mean) / jnp.maximum(1.0, upd_rms))
    for j in range(MATS):
        upd = grad[j] if j < WIDE else gsm[j - WIDE]
        new = weight_of(j) - scale[:, j:j + 1] * upd
        n, i = place(j)
        (w_in_n, w_out_n, w_qkv_n, w_o_n)[n][i] = new
    wait_for(sc_got.at[THREE], sent.at[SLABS + 1])


def write_out(*refs):
    n = len(refs) // 2
    copies = [pltpu.make_async_copy(refs[j], refs[n + j], refs[-1].at[j]) for j in range(n)]
    for cp in copies:
        cp.start()
    for cp in copies:
        cp.wait()


def solution(mesh):
    rows_data = (P('data', None, None, 'model'), P(None, 'data', 'model'), P(None, 'data'), P(None, 'model'))
    rows_model = (P('data', None, 'model', None), P(None, 'model', 'data'), P(None, 'model'), P(None, 'data'))
    DMA = pltpu.SemaphoreType.DMA

    def step_all(grad_in, w_in, row_in, col_in, grad_out, w_out, row_out, col_out,
                 grad_qkv, w_qkv, row_qkv, col_qkv, grad_o, w_o, row_o, col_o):
        args = (grad_in[0], w_in, row_in, col_in,
                grad_out[0], w_out.swapaxes(1, 2), row_out, col_out,
                grad_qkv[0].swapaxes(1, 2).reshape(-1, DIM), w_qkv, row_qkv, col_qkv,
                grad_o[0].reshape(-1, DIM), w_o.swapaxes(1, 2), row_o, col_o)
        small = [a for n, a in enumerate(args) if n % 4]
        outs = [jax.ShapeDtypeStruct(a.shape, a.dtype) for a in small]
        held = [pltpu.VMEM(a.shape, a.dtype) for a in small]
        vm = lambda *s: pltpu.VMEM(s, F32)
        res = pl.pallas_call(
            kernel,
            out_shape=held,
            in_specs=[pl.BlockSpec(memory_space=pl.ANY)] * len(args),
            out_specs=[pl.BlockSpec(memory_space=pltpu.VMEM)] * len(outs),
            scratch_shapes=[
                pltpu.VMEM((SLABS, DIM, DIM), jnp.bfloat16),
                vm(STEPS, 2, 4, 4, BLK, HALF), vm(STEPS, 2, 4, 4, BLK, HALF),
                vm(STEPS, 2, 2, 2, BLK, HALF), vm(STEPS, 2, 2, 4, BLK, HALF), vm(STEPS, 2, 4, BLK, HALF),
                vm(STEPS, 2, 2, 16, HALF), vm(STEPS, 2, 2, BLK, HALF),
                vm(SLABS, BLK, DIM), vm(12, BLK, THIN),
                vm(THIN, HALF), pltpu.VMEM((2, THIN, HALF), jnp.bfloat16)]
            + [vm(*a.shape) for n, a in enumerate(small) if n % 3 == 0] + [vm(*a.shape) for n, a in enumerate(small) if n % 3]
            + [vm(LANES, LANES), vm(16, PAIR), vm(16, PAIR), vm(BLK, LANES), vm(BLK, LANES),
               vm(len(GROUPS), BLK, LANES), vm(len(GROUPS), 4, BLK, LANES), vm(SLABS, 1, DIM), vm(SLABS, 1, DIM),
               vm(SLABS, 4, DIM), vm(SLABS, 8, 4, DIM), vm(SLABS, 4, DIM), vm(SLABS, 4, 4, DIM), vm(8, LANES), vm(4, 8, LANES),
               DMA((SLABS + 1 + 2 * PARTS,)), DMA((len(small),)), DMA((SLABS + 2,)), DMA((2, PARTS)), DMA((STEPS,)), DMA((STEPS,)), DMA((STEPS,)),
               DMA((len(GROUPS),)), DMA((1,))],
            compiler_params=pltpu.CompilerParams(
                collective_id=0, has_side_effects=True, vmem_limit_bytes=58_000_000),
            name='adafactor',
        )(*args)
        res = list(pl.pallas_call(
            write_out,
            out_shape=outs,
            in_specs=[pl.BlockSpec(memory_space=pltpu.VMEM)] * len(outs),
            out_specs=[pl.BlockSpec(memory_space=pl.ANY)] * len(outs),
            scratch_shapes=[DMA((len(outs),))],
            name='write_out',
        )(*[pltpu.with_memory_space_constraint(r, pltpu.VMEM) for r in res]))
        for n in (3, SLABS):
            res[n] = res[n].swapaxes(1, 2)
        return tuple(res)

    in_specs = rows_data + rows_model + rows_data + rows_model
    out_specs = rows_data[1:] + rows_model[1:] + rows_data[1:] + rows_model[1:]
    return jax.shard_map(step_all, mesh=mesh, in_specs=in_specs, out_specs=out_specs, check_vma=False)
```

```python
import jax
import jax.numpy as jnp
from jax import lax
from jax.experimental import pallas as pl
from jax.experimental.pallas import tpu as pltpu
from jax.sharding import PartitionSpec as P

OPT_STEP = 4
EPS_SQ = 1e-30
BETA_TWO = 1.0 - OPT_STEP ** -0.8
LR_BASE = min(1e-2, OPT_STEP ** -0.5)

F32 = jnp.float32
MESH = pl.DeviceIdType.MESH
FF, D = 3072.0, 768.0
DIM = 768
THIN = 192
LANES = 128
PAIR = 256
SLABS = 9
PLAIN = 4
WIDE = 6
MATS = 18
STEPS = SLABS
HALF = 384
BLK = 24
ROWCUT = (16, 8)
UP = 2.0 ** 48

GROUPS = tuple(range(n, min(n + 2, STEPS)) for n in range(0, STEPS, 2))
PARTS = 3


OTHERS = (1, 2, 3)
HALVES = range(2)
THREE, SEVEN = pl.ds(1, 3), pl.ds(1, 7)
DUO, TRIO, FOUR = pl.ds(0, 2), pl.ds(0, 3), pl.ds(0, 4)
FIRST, SECOND, THIRD, FOURTH = (slice(n, n + 1) for n in range(4))
IN, OUT, QKV, O = slice(4), slice(4, 6), slice(6, 15), slice(15, 18)


def down(v):
    return jnp.sum(v, axis=0, keepdims=True)


def along(v):
    return jnp.sum(v, axis=1, keepdims=True)


def mod4(v):
    return lax.rem(v + 8, 4)


def span(h, c):
    return pl.ds(HALF * h + LANES * c, LANES)


def cut(h, piece):
    return pl.ds(0, ROWCUT[h]) if piece == 0 else pl.ds(ROWCUT[h], BLK - ROWCUT[h])


def slab_of(s):
    if isinstance(s, int):
        return (0, 1, 6, 7, 8, 4, 5, 2, 3)[s]
    return jnp.where(s < 2, s, jnp.where(s < 5, s + 4, jnp.where(s < 7, s - 1, s - 5)))


def kernel(g_in, w_in, r_in, c_in, g_out, w_out, r_out, c_out, g_qkv, w_qkv, r_qkv, c_qkv, g_o, w_o, r_o, c_o,
           w_in_n, r_in_n, c_in_n, w_out_n, r_out_n, c_out_n, w_qkv_n, r_qkv_n, c_qkv_n, w_o_n, r_o_n, c_o_n,
           xin, s0, r0, r1a, r1b, b2, r2a, r2b, grad, gsm, pick_f, pick, vw_in, vw_out, vw_qkv, vw_o,
           vr_in, vc_in, vr_out, vc_out, vr_qkv, vc_qkv, vr_o, vc_o,
           square, thin_a, thin_b, dv_mom, dv_all, dv_own, dv_got, mv_mom, mv_new, mv_own, mv_y, mv_two, mv_z,
           sc_own, sc_got, ld_sem, sm_sem, sent, first_r, d2d_r, passed, whole, dv_r, sc_r, far):
    d = lax.axis_index('data')
    x = lax.axis_index('model')
    core = lax.rem(d, 2)
    y = lax.rem(d // 2, 4)
    z = d // 8

    def at(axis, off, other=0):
        if axis == 'x':
            return {'model': lax.rem(x + off, 4)}
        if axis == 'y':
            return {'data': (z * 4 + lax.rem(y + off, 4)) * 2 + (1 - core if other else core)}
        if axis == 'z':
            return {'data': (lax.rem(z + off, 4) * 4 + y) * 2 + core}
        return {'data': (z * 4 + y) * 2 + (1 - core)}

    def local(src, dst, sem):
        return pltpu.make_async_copy(src, dst, sem)

    loads = [None] + [local(g_in.at[k], xin.at[k], ld_sem.at[k]) for k in range(1, PLAIN)]
    loads += [local(g_out.at[k - PLAIN], xin.at[k], ld_sem.at[k]) for k in range(PLAIN, WIDE)]
    loads += [local(g_qkv.at[pl.ds(DIM * k, DIM)], xin.at[WIDE + k], ld_sem.at[WIDE + k]) for k in HALVES]
    loads += [local(g_qkv.at[pl.ds(2 * DIM, THIN)], xin.at[SLABS - 1, pl.ds(0, THIN)], ld_sem.at[SLABS - 1]),
              local(g_o, xin.at[SLABS - 1, pl.ds(THIN, DIM - THIN)], ld_sem.at[SLABS])]
    small = [(w_in, vw_in), (w_out, vw_out), (w_qkv, vw_qkv), (w_o, vw_o), (r_in, vr_in), (c_in, vc_in),
             (r_out, vr_out), (c_out, vc_out), (r_qkv, vr_qkv), (c_qkv, vc_qkv), (r_o, vr_o), (c_o, vc_o)]
    small = [local(s, t, sm_sem.at[j] if j < 6 else sent.at[j - 1]) for j, (s, t) in enumerate(small)]
    loads[0] = [local(g_in.at[0, :, span(h, c)], xin.at[0, :, span(h, c)], ld_sem.at[SLABS + 1 + h + 2 * c])
                for c in range(PARTS) for h in HALVES]
    for cp in loads[0] + [loads[1]]:
        cp.start()

    barrier = pltpu.get_barrier_semaphore()
    peers = [at('c', 1)] + [at(a, j) for a in 'yzx' for j in OTHERS if j % 2]
    for p in peers:
        pl.semaphore_signal(barrier, inc=1, device_id=p, device_id_type=MESH)

    def remote(src, dst, ss, rs, dev):
        return pltpu.make_async_remote_copy(src_ref=src, dst_ref=dst, send_sem=ss, recv_sem=rs,
                                            device_id=dev, device_id_type=MESH)

    def d2d(s, h):
        return remote(s0.at[s, h], r0.at[s, h], sent.at[0], d2d_r.at[s], at('c', 1))

    def make_pick():
        for side in HALVES:
            cc = (1 - core) if side == 0 else core
            row = lax.broadcasted_iota(jnp.int32, (BLK, HALF), 0)
            col = lax.broadcasted_iota(jnp.int32, (BLK, HALF), 1)
            for b in range(8):
                pick_f[pl.ds(BLK * b, BLK)] = jnp.where(col == row + 2 * BLK * b + BLK * cc, 1.0, 0.0)
            pick[side] = pick_f[...].astype(jnp.bfloat16)

    def part(s, h, side, fn, cols=None):
        k = slab_of(s)

        def plain():
            first = (core == 0) if side == 1 else (core == 1)
            for g in range(16):
                v = xin[k, pl.ds(2 * BLK * g, 2 * BLK), cols or pl.ds(HALF * h, HALF)].astype(F32)
                fn(pl.ds(g // 4, 1), pl.ds(g % 4, 1), jnp.where(first, v[:BLK], v[BLK:]).reshape(1, 1, BLK, -1))

        def turned():
            for g in HALVES:
                v = xin[k, pl.ds(HALF * h, HALF), pl.ds(HALF * g, HALF)]
                v = lax.dot_general(pick[side], v, (((1,), (1,)), ((), ())), preferred_element_type=F32)
                fn(pl.ds(2 * g, 2), slice(None), v.reshape(2, 4, BLK, HALF))
        choose(k < PLAIN, plain, turned)

    def choose(cond, yes, no):
        if isinstance(cond, bool):
            return yes() if cond else no()
        pl.when(cond)(yes)
        pl.when(jnp.logical_not(cond))(no)

    def stage_split(s):
        for j in range(1, SLABS):
            @pl.when(slab_of(s) == j)
            def _(j=j):
                loads[j].wait()
                if j == SLABS - 1:
                    loads[SLABS].wait()
        for h in HALVES:
            split_half(s, h)
            d2d(s, h).start()

    def split_half(s, h):
        def put(zs, ys, v):
            s0[s, h, zs, ys] = v
        part(s, h, 0, put)

    def first_d2d(h, c):
        cols = span(0, c)
        return remote(s0.at[0, h, :, :, :, cols], r0.at[0, h, :, :, :, cols], sent.at[0], first_r.at[h, c], at('c', 1))

    def ring(h, first):
        axis = ('y', 'z')[h] if first else ('z', 'y')[h]
        return axis, (y if axis == 'y' else z)

    def block(first, s, h, t, piece, flip):
        if not first:
            return b2.at[s, h, t, cut(h ^ flip, piece)]
        return r0.at[s, 0, pl.ds(2 * piece, 2), t] if h == 0 else r0.at[s, 1, t, pl.ds(2 * piece, 2)]

    PLAN = ((-2, 0, 0), (2, 1, 1), (-1, 1, 0), (1, 0, 1), (-1, 0, 0), (1, 1, 1))

    def passing(first, s, h, m, flip):
        _, piece, way = PLAN[m]
        return r1a.at[s, h, way] if first else r2a.at[s, h, way, pl.ds(0, cut(h ^ flip, piece).size)]

    def msg(first, s, h, m, flip, cols=slice(None)):
        axis, n = ring(h, first)
        off, piece, way = PLAN[m]
        landed = r1b if first else r2b
        src = block(first, s, h, mod4(n + off), piece, flip)
        if m < 2:
            dst = passing(first, s, h, m, flip)
        else:
            dst = landed.at[s, h, way, pl.ds(2 * piece, 2) if first else cut(h ^ flip, piece)]
        if first:
            src, dst = src.at[:, :, cols], dst.at[:, :, cols]
        return remote(src, dst, sent.at[1 if first else 2], passed.at[s] if m < 2 else whole.at[s] if first else d2d_r.at[s], at(axis, 1 if way else 3))

    def send_raw(first, s, h, flip, cols=slice(None)):
        for m in range(4):
            msg(first, s, h, m, flip, cols).start()

    def wait_for(ref, sem):
        local(ref, ref, sem).wait()

    def stage_add(s):
        wait_for(r0.at[s], d2d_r.at[s])
        for h in HALVES:

            def add(zs, ys, v, h=h):
                r0[s, h, zs, ys] += v
            part(s, h, 1, add)
            send_raw(True, s, h, 0)

    def first_split():
        for c in range(PARTS):
            for h in HALVES:
                def put(zs, ys, v, h=h, c=c):
                    s0[0, h, zs, ys, :, span(0, c)] = v
                loads[0][h + 2 * c].wait()
                part(0, h, 0, put, span(h, c))
                if h == 0 and c == 0:
                    pl.semaphore_wait(barrier, len(peers))
                first_d2d(h, c).start()

    def first_add():
        for c in range(PARTS):
            for h in HALVES:
                def add(zs, ys, v, h=h, c=c):
                    r0[0, h, zs, ys, :, span(0, c)] += v
                first_d2d(h, c).wait_recv()
                part(0, h, 1, add, span(h, c))
                send_raw(True, 0, h, 0, span(0, c))

    def relay(first, s, flip):
        wait_for(r1a.at[s] if first else b2.at[s, 0, DUO], passed.at[s])
        for h in HALVES:
            n = ring(h, first)[1]
            for m in HALVES:
                off, piece, _ = PLAN[4 + m]
                ref = block(first, s, h, mod4(n + off), piece, flip)
                ref[...] += passing(first, s, h, m, flip)[...]
                msg(first, s, h, 4 + m, flip).start()

    def stage_turn(s, flip):
        wait_for(r1b.at[s], whole.at[s])
        for h in HALVES:
            n = ring(h, True)[1]
            own = r0[s, 0, :, n] if h == 0 else r0[s, 1, n]
            b2[s, h] = own + r1b[s, h, 0] + r1b[s, h, 1]
            send_raw(False, s, h, flip)

    def stage_sum(s):
        wait_for(r2b.at[s], d2d_r.at[s])
        for h in HALVES:
            n = ring(h, False)[1]
            grad[slab_of(s), :, pl.ds(HALF * h, HALF)] = (b2[s, h, n] + r2b[s, h, 0] + r2b[s, h, 1]) / 32

    lane = lax.broadcasted_iota(jnp.int32, (1, LANES), 1)
    col = lax.broadcasted_iota(jnp.int32, (1, DIM), 1)
    count = jnp.where(lane < WIDE, FF, D)

    def of_mat(q):
        return jnp.logical_and(col >= THIN * q, col < THIN * q + THIN)

    def total(v):
        return along(down(v))

    def place(j):
        n = 0 if j < 4 else 1 if j < 6 else 2 if j < 15 else 3
        return n, j - (0, 4, 6, 15)[n]

    def weight_of(j):
        n, i = place(j)
        return (vw_in, vw_out, vw_qkv, vw_o)[n][i]

    def prepare():
        for cp in small:
            cp.wait()
        pl.semaphore_wait(far, 2)
        square[...] = jnp.zeros_like(square)
        square[IN, :BLK] = vr_in[...]
        square[OUT, :BLK] = vc_out[...]
        square[QKV, :BLK] = vr_qkv[...]
        square[O, :BLK] = vc_o[...]
        dv_mom[...] = square[...].T[:BLK]
        thin_a[...] = jnp.zeros_like(thin_a)
        thin_a[:9, :THIN] = vc_qkv[...]
        thin_a[9:12, :THIN] = vr_o[...]
        thin_b[...] = pltpu.roll(thin_a[...], 64, 1)
        for k in range(4):
            mv_mom[k] = vc_in[k:k + 1]
        for k in HALVES:
            mv_mom[4 + k] = vr_out[k:k + 1]
        for j in range(12):
            k, q = WIDE + j // 4, j % 4
            if q % 2 == 0:
                mv_mom[k, :, THIN * q:THIN * q + THIN] = thin_a[j:j + 1, :THIN]
            else:
                span = slice(THIN * q - 64, THIN * q + THIN)
                mv_mom[k, :, span] = jnp.where(col[:, :PAIR] < 64, mv_mom[k, :, span], thin_b[j:j + 1])
        mv_own[...] = jnp.zeros_like(mv_own)
        sc_own[...] = jnp.zeros_like(sc_own)
        dv_all[...] = jnp.ones_like(dv_all)
        vec = jnp.zeros((1, LANES), F32)
        for j in range(MATS):
            w = weight_of(j)
            vec = jnp.where(lane == j, total(w * w), vec)
        mv_own[slab_of(0), THIRD, LANES:PAIR] = vec
        mv_own[slab_of(0), THIRD, :LANES] = down(dv_mom[...])

    def spread(axis, src, dst, ss, rs):
        return [remote(src, dst.at[j], ss, rs, at(axis, j)) for j in OTHERS]

    def start(copies):
        for cp in copies:
            cp.start()

    def rows_of(k):
        return pl.ds(0, 3 if k == slab_of(0) else 2)

    def dv_copies(n):
        return spread('x', dv_own.at[n], dv_got.at[n], sent.at[3], dv_r.at[n])

    def y_copies(k):
        src = mv_own.at[k, rows_of(k)]
        return [remote(src, mv_y.at[k, j + 4 * other, rows_of(k)], sent.at[4 + rows_of(k).size], ld_sem.at[k],
                       at('y', j, other) if j else at('c', 1)) for j in range(4) for other in HALVES if j or other]

    def z_copies(k):
        return [remote(mv_two.at[k, rows_of(k)], mv_z.at[k, j, rows_of(k)], sent.at[6 + rows_of(k).size], whole.at[k], at('z', j))
                for j in OTHERS]

    def sums(k):
        g = grad[k]
        s = g * g + EPS_SQ
        if k < WIDE:
            return jnp.where(lane == k, along(s), 0.0)
        dv = jnp.zeros((BLK, LANES), F32)
        for q in range(4):
            low = HALF * (q // 2)
            t = jnp.where(of_mat(q)[:, low:low + HALF], s[:, low:low + HALF], 0.0)
            dv = jnp.where(lane == 4 * k - 18 + q, along(t), dv)
        return dv

    def mats_of(k):
        low, high = (k, k + 1) if k < WIDE else (4 * k - 18, 4 * k - 14)
        return jnp.logical_and(lane >= low, lane < high)

    def finish(n):
        dv = jnp.zeros((BLK, LANES), F32)
        for s in GROUPS[n]:
            stage_sum(s)
            dv = dv + sums(slab_of(s))
        dv_own[n] = dv
        start(dv_copies(n))
        for s in GROUPS[n]:
            k = slab_of(s)
            g = grad[k]
            mv_own[k, FIRST] = down(g * g + EPS_SQ)

    def data(n):
        wait_for(dv_got.at[n, THREE], dv_r.at[n])
        got = (dv_own[n] + dv_got[n, 2]) + (dv_got[n, 1] + dv_got[n, 3])
        new = BETA_TWO * dv_mom[...] + (1.0 - BETA_TWO) * (got / count)
        mine = lane < 0
        for s in GROUPS[n]:
            mine = jnp.logical_or(mine, mats_of(slab_of(s)))
        dv_all[...] = jnp.where(mine, new, dv_all[...])
        inv = 1.0 / jnp.sqrt(jnp.where(mine, new, 1.0))
        for s in GROUPS[n]:
            k = slab_of(s)
            if k < WIDE:
                factor = inv[:, k:k + 1]
            else:
                factor = inv[:, 4 * k - 15:4 * k - 14]
                for q in reversed(range(3)):
                    factor = jnp.where(col < THIN * q + THIN, inv[:, 4 * k - 18 + q:4 * k - 17 + q], factor)
            g = grad[k] * factor
            grad[k] = g
            g = g * UP
            mv_own[k, SECOND] = down(g * g)
            start(y_copies(k))

    def stage_z(k):
        wait_for(mv_y.at[k, SEVEN, rows_of(k)], ld_sem.at[k])
        one = [mv_own[k] + mv_y[k, 4]] + [mv_y[k, j] + mv_y[k, 4 + j] for j in OTHERS]
        mv_two[k] = (one[0] + one[2]) + (one[1] + one[3])
        start(z_copies(k))

    def model_side(k):
        mine = mats_of(k)
        wait_for(mv_z.at[k, THREE, rows_of(k)], whole.at[k])
        v = (mv_two[k] + mv_z[k, 2]) + (mv_z[k, 1] + mv_z[k, 3])
        new = BETA_TWO * mv_mom[k] + (1.0 - BETA_TWO) * (v[FIRST] / D)
        mv_new[k] = new
        inv = 1.0 / jnp.sqrt(new)
        a = jnp.sqrt(v[SECOND]) * inv * (1.0 / UP)
        a = a * a
        u = grad[k] * inv

        by_data = (1.0 - BETA_TWO) * (v[FIRST] / (FF if k < WIDE else D))

        def wide():
            sc_own[FIRST] = jnp.where(mine, total(a), sc_own[FIRST])
            sc_own[SECOND] = jnp.where(mine, total(by_data if k < 4 else new), sc_own[SECOND])
            grad[k] = u

        def thin():
            upd, row = sc_own[FIRST], sc_own[SECOND]
            for q in range(4):
                j = 4 * k - 18 + q
                upd = jnp.where(lane == j, total(jnp.where(of_mat(q), a, 0.0)), upd)
                row = jnp.where(lane == j, total(jnp.where(of_mat(q), by_data if j < 15 else new, 0.0)), row)
                if q % 2 == 0:
                    gsm[j - WIDE] = u[:, THIN * q:THIN * q + THIN]
                else:
                    gsm[j - WIDE] = pltpu.roll(u[:, THIN * q - 64:THIN * q + THIN], THIN, 1)[:, :THIN]
            sc_own[FIRST] = upd
            sc_own[SECOND] = row
        choose(k < WIDE, wide, thin)
        if rows_of(k).size == 3:
            sc_own[THIRD] = v[THIRD, LANES:PAIR]
            sc_own[FOURTH] = v[THIRD, :LANES]

    def turn(s):
        stage_turn(s, s % 2)

    def relay2(s):
        relay(False, s, s % 2)

    def relay1(s):
        relay(True, s, 0)

    def to_z(s):
        stage_z(slab_of(s))

    def model(s):
        model_side(slab_of(s))

    first_split()
    for j in OTHERS:
        if j % 2:
            pl.semaphore_signal(far, inc=1, device_id=at('x', j), device_id_type=MESH)
    for cp in [loads[slab_of(j)] for j in range(2, SLABS)] + loads[SLABS:] + small:
        cp.start()
    first_add()

    def trip(i, carry):
        @pl.when(i > 1)
        def _():
            stage_add(i - 1)
        stage_split(i)

        @pl.when(i > 1)
        def _():
            relay1(i - 2)

        @pl.when(i == 1)
        def _():
            make_pick()

        @pl.when(i == 3)
        def _():
            prepare()
        return carry
    lax.fori_loop(1, STEPS, trip, 0)

    def each(stage, steps):
        for s in steps:
            stage(s)

    last = STEPS - 1
    stage_add(last)
    relay1(last - 1)
    relay1(last)
    for stage in (turn, relay2):
        each(stage, range(STEPS))
    for stage in (finish, data):
        each(stage, range(len(GROUPS)))
    for stage in (to_z, model):
        each(stage, range(STEPS))

    sc_cp = [remote(sc_own.at[FOUR], sc_got.at[j, FOUR], sent.at[SLABS + 1], sc_r.at[0], at('x', j)) for j in OTHERS]
    start(sc_cp)

    square[:BLK] = dv_all[...]
    turned = square[...].T
    r_in_n[...] = turned[IN, :BLK]
    c_out_n[...] = turned[OUT, :BLK]
    r_qkv_n[...] = turned[QKV, :BLK]
    c_o_n[...] = turned[O, :BLK]
    for k in range(4):
        c_in_n[k:k + 1] = mv_new[k]
    for k in HALVES:
        r_out_n[k:k + 1] = mv_new[4 + k]
    for j in range(12):
        k, q = WIDE + j // 4, j % 4
        if q % 2 == 0:
            thin_a[j:j + 1, :THIN] = mv_new[k, :, THIN * q:THIN * q + THIN]
        else:
            thin_b[j:j + 1] = mv_new[k, :, THIN * q - 64:THIN * q + THIN]
    odd = lax.rem(lax.broadcasted_iota(jnp.int32, thin_a.shape, 0), 2) == 1
    thin_a[...] = jnp.where(odd, pltpu.roll(thin_b[...], THIN, 1), thin_a[...])
    c_qkv_n[...] = thin_a[:9, :THIN]
    r_o_n[...] = thin_a[9:12, :THIN]

    few = STEPS - 1
    for j, ref in enumerate((s0, s0.at[:, :, TRIO], b2.at[:, :, TRIO], dv_got.at[:, TRIO])):
        wait_for(ref, sent.at[j])
    wait_for(mv_y.at[pl.ds(0, few), SEVEN, DUO], sent.at[6])
    wait_for(mv_y.at[0, SEVEN, TRIO], sent.at[7])
    wait_for(mv_z.at[pl.ds(0, few), THREE, DUO], sent.at[8])
    wait_for(mv_z.at[0, THREE, TRIO], sent.at[9])

    wait_for(sc_got.at[THREE, FOUR], sc_r.at[0])
    sc = (sc_own[...] + sc_got[2]) + (sc_got[1] + sc_got[3])
    full = jnp.where(lane < WIDE, FF * D, D * D)
    rows = jnp.where(jnp.logical_and(lane >= 4, lane < 6), FF, D)
    by_model = jnp.logical_or(jnp.logical_and(lane >= 4, lane < 6), lane >= 15)
    row_mean = (sc[SECOND] + jnp.where(by_model, 0.0, BETA_TWO * (sc[FOURTH] / 4))) / rows
    upd_rms = jnp.sqrt(row_mean * (sc[FIRST] / full))
    w_rms = jnp.sqrt(sc[THIRD] / full)
    scale = LR_BASE * jnp.maximum(1e-3, w_rms) * (jnp.sqrt(row_mean) / jnp.maximum(1.0, upd_rms))
    for j in range(MATS):
        upd = grad[j] if j < WIDE else gsm[j - WIDE]
        new = weight_of(j) - scale[:, j:j + 1] * upd
        n, i = place(j)
        (w_in_n, w_out_n, w_qkv_n, w_o_n)[n][i] = new
    wait_for(sc_got.at[THREE, FOUR], sent.at[SLABS + 1])


def write_out(*refs):
    n = len(refs) // 2
    copies = [pltpu.make_async_copy(refs[j], refs[n + j], refs[-1].at[j]) for j in range(n)]
    for cp in copies:
        cp.start()
    for cp in copies:
        cp.wait()


def solution(mesh):
    rows_data = (P('data', None, None, 'model'), P(None, 'data', 'model'), P(None, 'data'), P(None, 'model'))
    rows_model = (P('data', None, 'model', None), P(None, 'model', 'data'), P(None, 'model'), P(None, 'data'))
    DMA = pltpu.SemaphoreType.DMA

    def step_all(grad_in, w_in, row_in, col_in, grad_out, w_out, row_out, col_out,
                 grad_qkv, w_qkv, row_qkv, col_qkv, grad_o, w_o, row_o, col_o):
        args = (grad_in[0], w_in, row_in, col_in,
                grad_out[0], w_out.swapaxes(1, 2), row_out, col_out,
                grad_qkv[0].swapaxes(1, 2).reshape(-1, DIM), w_qkv, row_qkv, col_qkv,
                grad_o[0].reshape(-1, DIM), w_o.swapaxes(1, 2), row_o, col_o)
        small = [a for n, a in enumerate(args) if n % 4]
        outs = [jax.ShapeDtypeStruct(a.shape, a.dtype) for a in small]
        held = [pltpu.VMEM(a.shape, a.dtype) for a in small]
        vm = lambda *s: pltpu.VMEM(s, F32)
        res = pl.pallas_call(
            kernel,
            out_shape=held,
            in_specs=[pl.BlockSpec(memory_space=pl.ANY)] * len(args),
            out_specs=[pl.BlockSpec(memory_space=pltpu.VMEM)] * len(outs),
            scratch_shapes=[
                pltpu.VMEM((SLABS, DIM, DIM), jnp.bfloat16),
                vm(STEPS, 2, 4, 4, BLK, HALF), vm(STEPS, 2, 4, 4, BLK, HALF),
                vm(STEPS, 2, 2, 2, BLK, HALF), vm(STEPS, 2, 2, 4, BLK, HALF), vm(STEPS, 2, 4, BLK, HALF),
                vm(STEPS, 2, 2, 16, HALF), vm(STEPS, 2, 2, BLK, HALF),
                vm(SLABS, BLK, DIM), vm(12, BLK, THIN),
                vm(THIN, HALF), pltpu.VMEM((2, THIN, HALF), jnp.bfloat16)]
            + [vm(*a.shape) for n, a in enumerate(small) if n % 3 == 0] + [vm(*a.shape) for n, a in enumerate(small) if n % 3]
            + [vm(LANES, LANES), vm(16, PAIR), vm(16, PAIR), vm(BLK, LANES), vm(BLK, LANES),
               vm(len(GROUPS), BLK, LANES), vm(len(GROUPS), 4, BLK, LANES), vm(SLABS, 1, DIM), vm(SLABS, 1, DIM),
               vm(SLABS, 4, DIM), vm(SLABS, 8, 4, DIM), vm(SLABS, 4, DIM), vm(SLABS, 4, 4, DIM), vm(8, LANES), vm(4, 8, LANES),
               DMA((SLABS + 1 + 2 * PARTS,)), DMA((6,)), DMA((SLABS + 2,)), DMA((2, PARTS)), DMA((STEPS,)), DMA((STEPS,)), DMA((STEPS,)),
               DMA((len(GROUPS),)), DMA((1,)), pltpu.SemaphoreType.REGULAR],
            compiler_params=pltpu.CompilerParams(
                collective_id=0, has_side_effects=True, vmem_limit_bytes=58_000_000),
            name='adafactor',
        )(*args)
        res = list(pl.pallas_call(
            write_out,
            out_shape=outs,
            in_specs=[pl.BlockSpec(memory_space=pltpu.VMEM)] * len(outs),
            out_specs=[pl.BlockSpec(memory_space=pl.ANY)] * len(outs),
            scratch_shapes=[DMA((len(outs),))],
            name='write_out',
        )(*[pltpu.with_memory_space_constraint(r, pltpu.VMEM) for r in res]))
        for n in (3, SLABS):
            res[n] = res[n].swapaxes(1, 2)
        return tuple(res)

    in_specs = rows_data + rows_model + rows_data + rows_model
    out_specs = rows_data[1:] + rows_model[1:] + rows_data[1:] + rows_model[1:]
    return jax.shard_map(step_all, mesh=mesh, in_specs=in_specs, out_specs=out_specs, check_vma=False)
```

```python
import jax
import jax.numpy as jnp
from jax import lax
from jax.experimental import pallas as pl
from jax.experimental.pallas import tpu as pltpu
from jax.sharding import PartitionSpec as P

OPT_STEP = 4
EPS_SQ = 1e-30
BETA_TWO = 1.0 - OPT_STEP ** -0.8
LR_BASE = min(1e-2, OPT_STEP ** -0.5)

F32 = jnp.float32
MESH = pl.DeviceIdType.MESH
FF, D = 3072.0, 768.0
DIM = 768
THIN = 192
LANES = 128
PAIR = 256
SLABS = 9
PLAIN = 4
WIDE = 6
MATS = 18
STEPS = SLABS
HALF = 384
BLK = 24
ROWCUT = (16, 8)
UP = 2.0 ** 48

GROUPS = tuple(range(n, min(n + 2, STEPS)) for n in range(0, STEPS, 2))
PARTS = 3


OTHERS = (2, 1, 3)
HALVES = range(2)
THREE, SEVEN = pl.ds(1, 3), pl.ds(1, 7)
DUO, TRIO, FOUR = pl.ds(0, 2), pl.ds(0, 3), pl.ds(0, 4)
FIRST, SECOND, THIRD, FOURTH = (slice(n, n + 1) for n in range(4))
IN, OUT, QKV, O = slice(4), slice(4, 6), slice(6, 15), slice(15, 18)


def down(v):
    return jnp.sum(v, axis=0, keepdims=True)


def along(v):
    return jnp.sum(v, axis=1, keepdims=True)


def mod4(v):
    return lax.rem(v + 8, 4)


def span(h, c):
    return pl.ds(HALF * h + LANES * c, LANES)


def cut(h, piece):
    return pl.ds(0, ROWCUT[h]) if piece == 0 else pl.ds(ROWCUT[h], BLK - ROWCUT[h])


def slab_of(s):
    if isinstance(s, int):
        return (0, 1, 6, 7, 8, 4, 5, 2, 3)[s]
    return jnp.where(s < 2, s, jnp.where(s < 5, s + 4, jnp.where(s < 7, s - 1, s - 5)))


def kernel(g_in, w_in, r_in, c_in, g_out, w_out, r_out, c_out, g_qkv, w_qkv, r_qkv, c_qkv, g_o, w_o, r_o, c_o,
           w_in_n, r_in_n, c_in_n, w_out_n, r_out_n, c_out_n, w_qkv_n, r_qkv_n, c_qkv_n, w_o_n, r_o_n, c_o_n,
           xin, s0, r0, r1a, r1b, b2, r2a, r2b, grad, gsm, pick_f, pick, vw_in, vw_out, vw_qkv, vw_o,
           vr_in, vc_in, vr_out, vc_out, vr_qkv, vc_qkv, vr_o, vc_o,
           square, thin_a, thin_b, dv_mom, dv_all, dv_own, dv_got, mv_mom, mv_new, mv_own, mv_y, mv_two, mv_z,
           sc_own, sc_got, ld_sem, sm_sem, sent, first_r, d2d_r, passed, whole, dv_r, sc_r, far):
    d = lax.axis_index('data')
    x = lax.axis_index('model')
    core = lax.rem(d, 2)
    y = lax.rem(d // 2, 4)
    z = d // 8

    def at(axis, off, other=0):
        if axis == 'x':
            return {'model': lax.rem(x + off, 4)}
        if axis == 'y':
            return {'data': (z * 4 + lax.rem(y + off, 4)) * 2 + (1 - core if other else core)}
        if axis == 'z':
            return {'data': (lax.rem(z + off, 4) * 4 + y) * 2 + core}
        return {'data': (z * 4 + y) * 2 + (1 - core)}

    def local(src, dst, sem):
        return pltpu.make_async_copy(src, dst, sem)

    loads = [None] + [local(g_in.at[k], xin.at[k], ld_sem.at[k]) for k in range(1, PLAIN)]
    loads += [local(g_out.at[k - PLAIN], xin.at[k], ld_sem.at[k]) for k in range(PLAIN, WIDE)]
    loads += [local(g_qkv.at[pl.ds(DIM * k, DIM)], xin.at[WIDE + k], ld_sem.at[WIDE + k]) for k in HALVES]
    loads += [local(g_qkv.at[pl.ds(2 * DIM, THIN)], xin.at[SLABS - 1, pl.ds(0, THIN)], ld_sem.at[SLABS - 1]),
              local(g_o, xin.at[SLABS - 1, pl.ds(THIN, DIM - THIN)], ld_sem.at[SLABS])]
    small = [(w_in, vw_in), (w_out, vw_out), (w_qkv, vw_qkv), (w_o, vw_o), (r_in, vr_in), (c_in, vc_in),
             (r_out, vr_out), (c_out, vc_out), (r_qkv, vr_qkv), (c_qkv, vc_qkv), (r_o, vr_o), (c_o, vc_o)]
    small = [local(s, t, sm_sem.at[j] if j < 6 else sent.at[j - 1]) for j, (s, t) in enumerate(small)]
    loads[0] = [local(g_in.at[0, :, span(h, c)], xin.at[0, :, span(h, c)], ld_sem.at[SLABS + 1 + h + 2 * c])
                for c in range(PARTS) for h in HALVES]
    for cp in loads[0] + [loads[1]]:
        cp.start()

    barrier = pltpu.get_barrier_semaphore()
    peers = [at('c', 1)] + [at(a, j) for a in 'yzx' for j in OTHERS if j % 2]
    for p in peers:
        pl.semaphore_signal(barrier, inc=1, device_id=p, device_id_type=MESH)

    def remote(src, dst, ss, rs, dev):
        return pltpu.make_async_remote_copy(src_ref=src, dst_ref=dst, send_sem=ss, recv_sem=rs,
                                            device_id=dev, device_id_type=MESH)

    def d2d(s, h):
        return remote(s0.at[s, h], r0.at[s, h], sent.at[0], d2d_r.at[s], at('c', 1))

    def make_pick():
        for side in HALVES:
            cc = (1 - core) if side == 0 else core
            row = lax.broadcasted_iota(jnp.int32, (BLK, HALF), 0)
            col = lax.broadcasted_iota(jnp.int32, (BLK, HALF), 1)
            for b in range(8):
                pick_f[pl.ds(BLK * b, BLK)] = jnp.where(col == row + 2 * BLK * b + BLK * cc, 1.0, 0.0)
            pick[side] = pick_f[...].astype(jnp.bfloat16)

    def part(s, h, side, fn, cols=None):
        k = slab_of(s)

        def plain():
            first = (core == 0) if side == 1 else (core == 1)
            for g in range(16):
                v = xin[k, pl.ds(2 * BLK * g, 2 * BLK), cols or pl.ds(HALF * h, HALF)].astype(F32)
                fn(pl.ds(g // 4, 1), pl.ds(g % 4, 1), jnp.where(first, v[:BLK], v[BLK:]).reshape(1, 1, BLK, -1))

        def turned():
            for g in HALVES:
                v = xin[k, pl.ds(HALF * h, HALF), pl.ds(HALF * g, HALF)]
                v = lax.dot_general(pick[side], v, (((1,), (1,)), ((), ())), preferred_element_type=F32)
                fn(pl.ds(2 * g, 2), slice(None), v.reshape(2, 4, BLK, HALF))
        choose(k < PLAIN, plain, turned)

    def choose(cond, yes, no):
        if isinstance(cond, bool):
            return yes() if cond else no()
        pl.when(cond)(yes)
        pl.when(jnp.logical_not(cond))(no)

    def stage_split(s):
        for j in range(1, SLABS):
            @pl.when(slab_of(s) == j)
            def _(j=j):
                loads[j].wait()
                if j == SLABS - 1:
                    loads[SLABS].wait()
        for h in HALVES:
            split_half(s, h)
            d2d(s, h).start()

    def split_half(s, h):
        def put(zs, ys, v):
            s0[s, h, zs, ys] = v
        part(s, h, 0, put)

    def first_d2d(h, c):
        cols = span(0, c)
        return remote(s0.at[0, h, :, :, :, cols], r0.at[0, h, :, :, :, cols], sent.at[0], first_r.at[h, c], at('c', 1))

    def ring(h, first):
        axis = ('y', 'z')[h] if first else ('z', 'y')[h]
        return axis, (y if axis == 'y' else z)

    def block(first, s, h, t, piece, flip):
        if not first:
            return b2.at[s, h, t, cut(h ^ flip, piece)]
        return r0.at[s, 0, pl.ds(2 * piece, 2), t] if h == 0 else r0.at[s, 1, t, pl.ds(2 * piece, 2)]

    PLAN = ((-2, 0, 0), (2, 1, 1), (-1, 1, 0), (1, 0, 1), (-1, 0, 0), (1, 1, 1))

    def passing(first, s, h, m, flip):
        _, piece, way = PLAN[m]
        return r1a.at[s, h, way] if first else r2a.at[s, h, way, pl.ds(0, cut(h ^ flip, piece).size)]

    def msg(first, s, h, m, flip, cols=slice(None)):
        axis, n = ring(h, first)
        off, piece, way = PLAN[m]
        landed = r1b if first else r2b
        src = block(first, s, h, mod4(n + off), piece, flip)
        if m < 2:
            dst = passing(first, s, h, m, flip)
        else:
            dst = landed.at[s, h, way, pl.ds(2 * piece, 2) if first else cut(h ^ flip, piece)]
        if first:
            src, dst = src.at[:, :, cols], dst.at[:, :, cols]
        return remote(src, dst, sent.at[1 if first else 2], passed.at[s] if m < 2 else whole.at[s] if first else d2d_r.at[s], at(axis, 1 if way else 3))

    def send_raw(first, s, h, flip, cols=slice(None)):
        for m in range(4):
            msg(first, s, h, m, flip, cols).start()

    def wait_for(ref, sem):
        local(ref, ref, sem).wait()

    def stage_add(s):
        wait_for(r0.at[s], d2d_r.at[s])
        for h in HALVES:

            def add(zs, ys, v, h=h):
                r0[s, h, zs, ys] += v
            part(s, h, 1, add)
            send_raw(True, s, h, 0)

    def first_split():
        for c in range(PARTS):
            for h in HALVES:
                def put(zs, ys, v, h=h, c=c):
                    s0[0, h, zs, ys, :, span(0, c)] = v
                loads[0][h + 2 * c].wait()
                part(0, h, 0, put, span(h, c))
                if h == 0 and c == 0:
                    pl.semaphore_wait(barrier, len(peers))
                first_d2d(h, c).start()

    def first_add():
        for c in range(PARTS):
            for h in HALVES:
                def add(zs, ys, v, h=h, c=c):
                    r0[0, h, zs, ys, :, span(0, c)] += v
                first_d2d(h, c).wait_recv()
                part(0, h, 1, add, span(h, c))
                send_raw(True, 0, h, 0, span(0, c))

    def relay(first, s, flip):
        wait_for(r1a.at[s] if first else b2.at[s, 0, DUO], passed.at[s])
        for h in HALVES:
            n = ring(h, first)[1]
            for m in HALVES:
                off, piece, _ = PLAN[4 + m]
                ref = block(first, s, h, mod4(n + off), piece, flip)
                ref[...] += passing(first, s, h, m, flip)[...]
                msg(first, s, h, 4 + m, flip).start()

    def stage_turn(s, flip):
        wait_for(r1b.at[s], whole.at[s])
        for h in HALVES:
            n = ring(h, True)[1]
            own = r0[s, 0, :, n] if h == 0 else r0[s, 1, n]
            b2[s, h] = own + r1b[s, h, 0] + r1b[s, h, 1]
            send_raw(False, s, h, flip)

    def stage_sum(s):
        wait_for(r2b.at[s], d2d_r.at[s])
        for h in HALVES:
            n = ring(h, False)[1]
            grad[slab_of(s), :, pl.ds(HALF * h, HALF)] = (b2[s, h, n] + r2b[s, h, 0] + r2b[s, h, 1]) / 32

    lane = lax.broadcasted_iota(jnp.int32, (1, LANES), 1)
    col = lax.broadcasted_iota(jnp.int32, (1, DIM), 1)
    count = jnp.where(lane < WIDE, FF, D)

    def of_mat(q):
        return jnp.logical_and(col >= THIN * q, col < THIN * q + THIN)

    def total(v):
        return along(down(v))

    def place(j):
        n = 0 if j < 4 else 1 if j < 6 else 2 if j < 15 else 3
        return n, j - (0, 4, 6, 15)[n]

    def weight_of(j):
        n, i = place(j)
        return (vw_in, vw_out, vw_qkv, vw_o)[n][i]

    def prepare():
        for cp in small:
            cp.wait()
        pl.semaphore_wait(far, 2)
        square[...] = jnp.zeros_like(square)
        square[IN, :BLK] = vr_in[...]
        square[OUT, :BLK] = vc_out[...]
        square[QKV, :BLK] = vr_qkv[...]
        square[O, :BLK] = vc_o[...]
        dv_mom[...] = square[...].T[:BLK]
        thin_a[...] = jnp.zeros_like(thin_a)
        thin_a[:9, :THIN] = vc_qkv[...]
        thin_a[9:12, :THIN] = vr_o[...]
        thin_b[...] = pltpu.roll(thin_a[...], 64, 1)
        for k in range(4):
            mv_mom[k] = vc_in[k:k + 1]
        for k in HALVES:
            mv_mom[4 + k] = vr_out[k:k + 1]
        for j in range(12):
            k, q = WIDE + j // 4, j % 4
            if q % 2 == 0:
                mv_mom[k, :, THIN * q:THIN * q + THIN] = thin_a[j:j + 1, :THIN]
            else:
                span = slice(THIN * q - 64, THIN * q + THIN)
                mv_mom[k, :, span] = jnp.where(col[:, :PAIR] < 64, mv_mom[k, :, span], thin_b[j:j + 1])
        mv_own[...] = jnp.zeros_like(mv_own)
        sc_own[...] = jnp.zeros_like(sc_own)
        dv_all[...] = jnp.ones_like(dv_all)
        vec = jnp.zeros((1, LANES), F32)
        for j in range(MATS):
            w = weight_of(j)
            vec = jnp.where(lane == j, total(w * w), vec)
        mv_own[slab_of(0), THIRD, LANES:PAIR] = vec
        mv_own[slab_of(0), THIRD, :LANES] = down(dv_mom[...])

    def spread(axis, src, dst, ss, rs):
        return [remote(src, dst.at[j], ss, rs, at(axis, j)) for j in OTHERS]

    def start(copies):
        for cp in copies:
            cp.start()

    def rows_of(k):
        return pl.ds(0, 3 if k == slab_of(0) else 2)

    def dv_copies(n):
        return spread('x', dv_own.at[n], dv_got.at[n], sent.at[3], dv_r.at[n])

    def y_copies(k):
        src = mv_own.at[k, rows_of(k)]
        return [remote(src, mv_y.at[k, j + 4 * other, rows_of(k)], sent.at[4 + rows_of(k).size], ld_sem.at[k],
                       at('y', j, other) if j else at('c', 1)) for j in OTHERS + (0,) for other in HALVES if j or other]

    def z_copies(k):
        return [remote(mv_two.at[k, rows_of(k)], mv_z.at[k, j, rows_of(k)], sent.at[6 + rows_of(k).size], whole.at[k], at('z', j))
                for j in OTHERS]

    def sums(k):
        g = grad[k]
        s = g * g + EPS_SQ
        if k < WIDE:
            return jnp.where(lane == k, along(s), 0.0)
        dv = jnp.zeros((BLK, LANES), F32)
        for q in range(4):
            low = HALF * (q // 2)
            t = jnp.where(of_mat(q)[:, low:low + HALF], s[:, low:low + HALF], 0.0)
            dv = jnp.where(lane == 4 * k - 18 + q, along(t), dv)
        return dv

    def mats_of(k):
        low, high = (k, k + 1) if k < WIDE else (4 * k - 18, 4 * k - 14)
        return jnp.logical_and(lane >= low, lane < high)

    def finish(n):
        dv = jnp.zeros((BLK, LANES), F32)
        for s in GROUPS[n]:
            stage_sum(s)
            dv = dv + sums(slab_of(s))
        dv_own[n] = dv
        start(dv_copies(n))
        for s in GROUPS[n]:
            k = slab_of(s)
            g = grad[k]
            mv_own[k, FIRST] = down(g * g + EPS_SQ)

    def data(n):
        wait_for(dv_got.at[n, THREE], dv_r.at[n])
        got = (dv_own[n] + dv_got[n, 2]) + (dv_got[n, 1] + dv_got[n, 3])
        new = BETA_TWO * dv_mom[...] + (1.0 - BETA_TWO) * (got / count)
        mine = lane < 0
        for s in GROUPS[n]:
            mine = jnp.logical_or(mine, mats_of(slab_of(s)))
        dv_all[...] = jnp.where(mine, new, dv_all[...])
        inv = 1.0 / jnp.sqrt(jnp.where(mine, new, 1.0))
        for s in GROUPS[n]:
            k = slab_of(s)
            if k < WIDE:
                factor = inv[:, k:k + 1]
            else:
                factor = inv[:, 4 * k - 15:4 * k - 14]
                for q in reversed(range(3)):
                    factor = jnp.where(col < THIN * q + THIN, inv[:, 4 * k - 18 + q:4 * k - 17 + q], factor)
            g = grad[k] * factor
            grad[k] = g
            g = g * UP
            mv_own[k, SECOND] = down(g * g)
            start(y_copies(k))

    def stage_z(k):
        wait_for(mv_y.at[k, SEVEN, rows_of(k)], ld_sem.at[k])
        one = [mv_own[k] + mv_y[k, 4]] + [mv_y[k, j] + mv_y[k, 4 + j] for j in sorted(OTHERS)]
        mv_two[k] = (one[0] + one[2]) + (one[1] + one[3])
        start(z_copies(k))

    def model_side(k):
        mine = mats_of(k)
        wait_for(mv_z.at[k, THREE, rows_of(k)], whole.at[k])
        v = (mv_two[k] + mv_z[k, 2]) + (mv_z[k, 1] + mv_z[k, 3])
        new = BETA_TWO * mv_mom[k] + (1.0 - BETA_TWO) * (v[FIRST] / D)
        mv_new[k] = new
        inv = 1.0 / jnp.sqrt(new)
        a = jnp.sqrt(v[SECOND]) * inv * (1.0 / UP)
        a = a * a
        u = grad[k] * inv

        by_data = (1.0 - BETA_TWO) * (v[FIRST] / (FF if k < WIDE else D))

        def wide():
            sc_own[FIRST] = jnp.where(mine, total(a), sc_own[FIRST])
            sc_own[SECOND] = jnp.where(mine, total(by_data if k < 4 else new), sc_own[SECOND])
            grad[k] = u

        def thin():
            upd, row = sc_own[FIRST], sc_own[SECOND]
            for q in range(4):
                j = 4 * k - 18 + q
                upd = jnp.where(lane == j, total(jnp.where(of_mat(q), a, 0.0)), upd)
                row = jnp.where(lane == j, total(jnp.where(of_mat(q), by_data if j < 15 else new, 0.0)), row)
                if q % 2 == 0:
                    gsm[j - WIDE] = u[:, THIN * q:THIN * q + THIN]
                else:
                    gsm[j - WIDE] = pltpu.roll(u[:, THIN * q - 64:THIN * q + THIN], THIN, 1)[:, :THIN]
            sc_own[FIRST] = upd
            sc_own[SECOND] = row
        choose(k < WIDE, wide, thin)
        if rows_of(k).size == 3:
            sc_own[THIRD] = v[THIRD, LANES:PAIR]
            sc_own[FOURTH] = v[THIRD, :LANES]

    def turn(s):
        stage_turn(s, s % 2)

    def relay2(s):
        relay(False, s, s % 2)

    def relay1(s):
        relay(True, s, 0)

    def to_z(s):
        stage_z(slab_of(s))

    def model(s):
        model_side(slab_of(s))

    first_split()
    for j in OTHERS:
        if j % 2:
            pl.semaphore_signal(far, inc=1, device_id=at('x', j), device_id_type=MESH)
    for cp in [loads[slab_of(j)] for j in range(2, SLABS)] + loads[SLABS:] + small:
        cp.start()
    first_add()

    def trip(i, carry):
        @pl.when(i > 1)
        def _():
            stage_add(i - 1)
        stage_split(i)

        @pl.when(i > 1)
        def _():
            relay1(i - 2)

        @pl.when(i == 1)
        def _():
            make_pick()

        @pl.when(i == 3)
        def _():
            prepare()
        return carry
    lax.fori_loop(1, STEPS, trip, 0)

    def each(stage, steps):
        for s in steps:
            stage(s)

    last = STEPS - 1
    stage_add(last)
    relay1(last - 1)
    relay1(last)
    for stage in (turn, relay2):
        each(stage, range(STEPS))
    for stage in (finish, data):
        each(stage, range(len(GROUPS)))
    for stage in (to_z, model):
        each(stage, range(STEPS))

    sc_cp = [remote(sc_own.at[FOUR], sc_got.at[j, FOUR], sent.at[SLABS + 1], sc_r.at[0], at('x', j)) for j in OTHERS]
    start(sc_cp)

    square[:BLK] = dv_all[...]
    turned = square[...].T
    r_in_n[...] = turned[IN, :BLK]
    c_out_n[...] = turned[OUT, :BLK]
    r_qkv_n[...] = turned[QKV, :BLK]
    c_o_n[...] = turned[O, :BLK]
    for k in range(4):
        c_in_n[k:k + 1] = mv_new[k]
    for k in HALVES:
        r_out_n[k:k + 1] = mv_new[4 + k]
    for j in range(12):
        k, q = WIDE + j // 4, j % 4
        if q % 2 == 0:
            thin_a[j:j + 1, :THIN] = mv_new[k, :, THIN * q:THIN * q + THIN]
        else:
            thin_b[j:j + 1] = mv_new[k, :, THIN * q - 64:THIN * q + THIN]
    odd = lax.rem(lax.broadcasted_iota(jnp.int32, thin_a.shape, 0), 2) == 1
    thin_a[...] = jnp.where(odd, pltpu.roll(thin_b[...], THIN, 1), thin_a[...])
    c_qkv_n[...] = thin_a[:9, :THIN]
    r_o_n[...] = thin_a[9:12, :THIN]

    few = STEPS - 1
    for j, ref in enumerate((s0, s0.at[:, :, TRIO], b2.at[:, :, TRIO], dv_got.at[:, TRIO])):
        wait_for(ref, sent.at[j])
    wait_for(mv_y.at[pl.ds(0, few), SEVEN, DUO], sent.at[6])
    wait_for(mv_y.at[0, SEVEN, TRIO], sent.at[7])
    wait_for(mv_z.at[pl.ds(0, few), THREE, DUO], sent.at[8])
    wait_for(mv_z.at[0, THREE, TRIO], sent.at[9])

    wait_for(sc_got.at[THREE, FOUR], sc_r.at[0])
    sc = (sc_own[...] + sc_got[2]) + (sc_got[1] + sc_got[3])
    full = jnp.where(lane < WIDE, FF * D, D * D)
    rows = jnp.where(jnp.logical_and(lane >= 4, lane < 6), FF, D)
    by_model = jnp.logical_or(jnp.logical_and(lane >= 4, lane < 6), lane >= 15)
    row_mean = (sc[SECOND] + jnp.where(by_model, 0.0, BETA_TWO * (sc[FOURTH] / 4))) / rows
    upd_rms = jnp.sqrt(row_mean * (sc[FIRST] / full))
    w_rms = jnp.sqrt(sc[THIRD] / full)
    scale = LR_BASE * jnp.maximum(1e-3, w_rms) * (jnp.sqrt(row_mean) / jnp.maximum(1.0, upd_rms))
    for j in range(MATS):
        upd = grad[j] if j < WIDE else gsm[j - WIDE]
        new = weight_of(j) - scale[:, j:j + 1] * upd
        n, i = place(j)
        (w_in_n, w_out_n, w_qkv_n, w_o_n)[n][i] = new
    wait_for(sc_got.at[THREE, FOUR], sent.at[SLABS + 1])


def write_out(*refs):
    n = len(refs) // 2
    copies = [pltpu.make_async_copy(refs[j], refs[n + j], refs[-1].at[j]) for j in range(n)]
    for cp in copies:
        cp.start()
    for cp in copies:
        cp.wait()


def solution(mesh):
    rows_data = (P('data', None, None, 'model'), P(None, 'data', 'model'), P(None, 'data'), P(None, 'model'))
    rows_model = (P('data', None, 'model', None), P(None, 'model', 'data'), P(None, 'model'), P(None, 'data'))
    DMA = pltpu.SemaphoreType.DMA

    def step_all(grad_in, w_in, row_in, col_in, grad_out, w_out, row_out, col_out,
                 grad_qkv, w_qkv, row_qkv, col_qkv, grad_o, w_o, row_o, col_o):
        args = (grad_in[0], w_in, row_in, col_in,
                grad_out[0], w_out.swapaxes(1, 2), row_out, col_out,
                grad_qkv[0].swapaxes(1, 2).reshape(-1, DIM), w_qkv, row_qkv, col_qkv,
                grad_o[0].reshape(-1, DIM), w_o.swapaxes(1, 2), row_o, col_o)
        small = [a for n, a in enumerate(args) if n % 4]
        outs = [jax.ShapeDtypeStruct(a.shape, a.dtype) for a in small]
        held = [pltpu.VMEM(a.shape, a.dtype) for a in small]
        vm = lambda *s: pltpu.VMEM(s, F32)
        res = pl.pallas_call(
            kernel,
            out_shape=held,
            in_specs=[pl.BlockSpec(memory_space=pl.ANY)] * len(args),
            out_specs=[pl.BlockSpec(memory_space=pltpu.VMEM)] * len(outs),
            scratch_shapes=[
                pltpu.VMEM((SLABS, DIM, DIM), jnp.bfloat16),
                vm(STEPS, 2, 4, 4, BLK, HALF), vm(STEPS, 2, 4, 4, BLK, HALF),
                vm(STEPS, 2, 2, 2, BLK, HALF), vm(STEPS, 2, 2, 4, BLK, HALF), vm(STEPS, 2, 4, BLK, HALF),
                vm(STEPS, 2, 2, 16, HALF), vm(STEPS, 2, 2, BLK, HALF),
                vm(SLABS, BLK, DIM), vm(12, BLK, THIN),
                vm(THIN, HALF), pltpu.VMEM((2, THIN, HALF), jnp.bfloat16)]
            + [vm(*a.shape) for n, a in enumerate(small) if n % 3 == 0] + [vm(*a.shape) for n, a in enumerate(small) if n % 3]
            + [vm(LANES, LANES), vm(16, PAIR), vm(16, PAIR), vm(BLK, LANES), vm(BLK, LANES),
               vm(len(GROUPS), BLK, LANES), vm(len(GROUPS), 4, BLK, LANES), vm(SLABS, 1, DIM), vm(SLABS, 1, DIM),
               vm(SLABS, 4, DIM), vm(SLABS, 8, 4, DIM), vm(SLABS, 4, DIM), vm(SLABS, 4, 4, DIM), vm(8, LANES), vm(4, 8, LANES),
               DMA((SLABS + 1 + 2 * PARTS,)), DMA((6,)), DMA((SLABS + 2,)), DMA((2, PARTS)), DMA((STEPS,)), DMA((STEPS,)), DMA((STEPS,)),
               DMA((len(GROUPS),)), DMA((1,)), pltpu.SemaphoreType.REGULAR],
            compiler_params=pltpu.CompilerParams(
                collective_id=0, has_side_effects=True, vmem_limit_bytes=58_000_000),
            name='adafactor',
        )(*args)
        res = list(pl.pallas_call(
            write_out,
            out_shape=outs,
            in_specs=[pl.BlockSpec(memory_space=pltpu.VMEM)] * len(outs),
            out_specs=[pl.BlockSpec(memory_space=pl.ANY)] * len(outs),
            scratch_shapes=[DMA((len(outs),))],
            name='write_out',
        )(*[pltpu.with_memory_space_constraint(r, pltpu.VMEM) for r in res]))
        for n in (3, SLABS):
            res[n] = res[n].swapaxes(1, 2)
        return tuple(res)

    in_specs = rows_data + rows_model + rows_data + rows_model
    out_specs = rows_data[1:] + rows_model[1:] + rows_data[1:] + rows_model[1:]
    return jax.shard_map(step_all, mesh=mesh, in_specs=in_specs, out_specs=out_specs, check_vma=False)
```
